32 devices in a mesh: row: 8 (over y, x, core), col: 4 (over z).
Axes of the slice: x: 2, y: 2, z: 4, core: 2. Of those that a mesh axis runs over, the one named last changes fastest.
Arguments:
- features: bfloat16 [32768, 512], P('col', 'row'), may hold values from -6 to 6
- weight_t: bfloat16 [512, 512], P(None, 'row'), may hold values from -0.25 to 0.25
- tiles: bfloat16 [8192, 128, 128], P(('row', 'col')), may hold values from -0.15625 to 0.15625
- coords: int32 [2, 8192], P(None, ('row', 'col')), may hold values from 0 to 63, as said below
- counts: int32 [32], P(('row', 'col')), may hold values from 32 to 256, as said below
Outputs:
- output: bfloat16 [32768, 512], P('row', 'col')
The draws below stay inside these ranges and needn't reach their ends.
Inputs may be any that keep to these rules, and one draw needn't show every extreme that they name: coords[0] of a slot lies in 0 to 31 and coords[1] in 0 to 63; the live slots of one grid cell name distinct tiles. `counts`: some grid cell has all 256 slots live in every draw.
All inputs are finite; a program needn't handle non-finite values.
Results may differ from the reference program's by a relative error of at most 0.0095.
Values may be sent and summed in bfloat16 or wider, within the bound.
A program may use at most 128 MiB of HBM per device.

```python
import jax
import jax.numpy as jnp
from jax import lax

TILE = 128
FEAT = 512
F_OUT = 512
TROW = 32
MAXT = 256
TCOL = 64
NODES = 32768
N_COL = 4
DEVICES = 32


def draw_coords(key, part):
    keys = jax.random.split(jax.random.fold_in(key, 11), DEVICES)
    spots = jax.vmap(lambda k: jax.random.permutation(k, TROW * TCOL)[:MAXT])(keys)
    spots = spots.reshape(DEVICES * MAXT).astype(jnp.int32)
    return jnp.stack([spots // TCOL, spots % TCOL]).astype(jnp.int32)


def draw_counts(key, part):
    base = jax.random.randint(jax.random.fold_in(key, 21), (DEVICES,), MAXT // 8, MAXT // 2 + 1)
    heavy = jax.random.randint(jax.random.fold_in(key, 22), (DEVICES,), 0, 8) == 0
    chosen = jax.random.randint(jax.random.fold_in(key, 23), (), 0, DEVICES)
    heavy = heavy | (jnp.arange(DEVICES, dtype=jnp.int32) == chosen)
    return jnp.where(heavy, MAXT, base).astype(jnp.int32)


def level_of(key, shape, cuts, least, high):
    level, own = 1.0, jax.random.fold_in(key, 6)
    for axis_at, parts in cuts:
        heights = jnp.exp(jax.random.uniform(jax.random.fold_in(own, axis_at), (parts,), jnp.float32, least / len(cuts), high / len(cuts)))
        level = level * jnp.repeat(heights, shape[axis_at] // parts).reshape([-1 if axis == axis_at else 1 for axis in range(len(shape))])
    return level


def scatter_about(key, dims, deviation, limit, pieces=(), kind=jnp.bfloat16):
    values = deviation * jax.random.normal(key, dims, jnp.float32)
    if pieces:
        values = values * level_of(key, dims, pieces, -0.22, 0.18)
    return jnp.clip(values, -limit, limit).astype(kind)


def setup_inputs(seed: int = 0) -> dict:
    streams_of = jax.random.split(jax.random.key(seed), 6)
    return {
        "features": scatter_about(streams_of[0], (NODES, FEAT), 1.0, 6.0, ((0, 4), (1, 8))),
        "weight_t": scatter_about(streams_of[1], (F_OUT, FEAT), FEAT ** -0.5, 0.25, ((1, 8),)),
        "tiles": scatter_about(streams_of[2], (DEVICES * MAXT, TILE, TILE), (2 * MAXT * TILE * N_COL // (5 * TROW)) ** -0.5, 0.15625, ((0, 32),)),
        "coords": draw_coords(jax.random.fold_in(streams_of[5], 71), 0),
        "counts": draw_counts(jax.random.fold_in(streams_of[5], 71), 0),
    }


def reference(features, weight_t, tiles, coords, counts):
    feat = features.shape[1]
    cblock = TCOL * TILE
    rblock = TROW * TILE
    lanes = jnp.arange(TROW, dtype=jnp.int32)
    slots = jnp.arange(MAXT, dtype=jnp.int32)

    def device(total, cell):
        rpos = cell // N_COL
        cpos = cell % N_COL
        block = lax.dynamic_slice_in_dim(tiles, (cell * MAXT).astype(jnp.int32), MAXT, 0).astype(jnp.float32)
        place = lax.dynamic_slice_in_dim(coords, (cell * MAXT).astype(jnp.int32), MAXT, 1)
        live = (slots < counts[cell]).astype(jnp.float32)
        panel = lax.dynamic_slice_in_dim(features, (cpos * cblock).astype(jnp.int32), cblock, 0)
        panel = panel.astype(jnp.float32).reshape(TCOL, TILE, feat)
        picked = panel[place[1]]
        prod = jnp.einsum('gij,gjw->giw', block * live[:, None, None], picked, precision=lax.Precision.HIGHEST)
        select = (place[0][:, None] == lanes[None, :]).astype(jnp.float32)
        part = jnp.einsum('gt,giw->tiw', select, prod, precision=lax.Precision.HIGHEST).reshape(rblock, feat)
        start = (rpos * rblock).astype(jnp.int32)
        old = lax.dynamic_slice_in_dim(total, start, rblock, 0)
        return lax.dynamic_update_slice_in_dim(total, old + part, start, 0), None

    total = jnp.zeros((NODES, feat), jnp.float32)
    total, _ = lax.scan(device, total, jnp.arange(DEVICES, dtype=jnp.int32))
    result = jnp.dot(total, weight_t.astype(jnp.float32).T, precision=lax.Precision.HIGHEST)
    return result.astype(jnp.bfloat16)
```

```python
import functools

import jax
import jax.numpy as jnp
from jax import lax
from jax.experimental import pallas as pl
from jax.experimental.pallas import tpu as pltpu
from jax.sharding import PartitionSpec as P

BUNCH = 4
PIECES = 8
EARLY = 2
VMEM_LIMIT = 62 * 1024 * 1024


def remote(src, dst, send, recv, axis, to):
    return pltpu.make_async_remote_copy(
        src_ref=src,
        dst_ref=dst,
        send_sem=send,
        recv_sem=recv,
        device_id={axis: to},
        device_id_type=pl.DeviceIdType.MESH,
    )


def plan_kernel(coords_ref, counts_ref, slots_ref, cols_ref, keep_ref, last_ref, lengths, bases):
    maxt = coords_ref.shape[1]
    trow = last_ref.shape[0]
    bunches = keep_ref.shape[0] - 1
    count = counts_ref[0]

    def clear_row(row, carry):
        lengths[row] = 0
        return carry

    lax.fori_loop(0, trow, clear_row, 0)

    def clear_slot(at, carry):
        slots_ref[at] = maxt
        cols_ref[at] = 0
        return carry

    lax.fori_loop(0, slots_ref.shape[0], clear_slot, 0, unroll=8)

    def clear_start(at, carry):
        keep_ref[at] = 1.0
        return carry

    lax.fori_loop(0, bunches, clear_start, 0, unroll=8)

    def tally(slot, carry):
        row = coords_ref[0, slot]
        lengths[row] = lengths[row] + 1
        return carry

    lax.fori_loop(0, count, tally, 0)

    def lay(row, base):
        need = (lengths[row] + BUNCH - 1) // BUNCH
        bases[row] = base * BUNCH
        keep_ref[jnp.where(need > 0, base, bunches)] = 0.0
        last_ref[row] = jnp.where(need > 0, base + need - 1, bunches)
        return base + need

    lax.fori_loop(0, trow, lay, 0)

    def enter(slot, carry):
        row = coords_ref[0, slot]
        at = bases[row]
        slots_ref[at] = slot
        cols_ref[at] = coords_ref[1, slot]
        bases[row] = at + 1
        return carry

    lax.fori_loop(0, count, enter, 0)


def plan(coords, counts, trow, bunches):
    smem = pl.BlockSpec(memory_space=pltpu.SMEM)
    return pl.pallas_call(
        plan_kernel,
        out_shape=[
            jax.ShapeDtypeStruct((bunches * BUNCH,), jnp.int32),
            jax.ShapeDtypeStruct((bunches * BUNCH,), jnp.int32),
            jax.ShapeDtypeStruct((bunches + 1,), jnp.float32),
            jax.ShapeDtypeStruct((trow,), jnp.int32),
        ],
        in_specs=[smem] * 2,
        out_specs=[smem] * 4,
        scratch_shapes=[pltpu.SMEM((trow,), jnp.int32), pltpu.SMEM((trow,), jnp.int32)],
        name="plan",
    )(coords, counts)


def layer_kernel(rows_n, parts, slots_ref, cols_ref, keep_ref, last_ref, f_ref, w_ref, tiles_hbm, out_ref,
                 tiles_ref, ft, xs, w_mine, weights, panels, runs, partial, landed,
                 tiles_sem, f_send, f_recv, w_send, w_recv, h_send, h_recv, sib_send, z_send, z_recv):
    me = lax.axis_index("row")
    here = lax.axis_index("col")
    maxt, tile, _ = tiles_hbm.shape
    fw, nodes = f_ref.shape
    block = nodes // rows_n
    deep = block // tile
    width = out_ref.shape[1]
    rows = out_ref.shape[0]
    feat = rows_n * fw
    bunches = keep_ref.shape[0] - 1
    trow = last_ref.shape[0]
    core = me % 2
    sibling = me + 1 - 2 * core
    twins = rows_n // 2

    fetch = pltpu.make_async_copy(tiles_hbm, tiles_ref.at[pl.ds(0, maxt)], tiles_sem)
    fetch.start()

    barrier = pltpu.get_barrier_semaphore()
    for step in range(1, rows_n):
        pl.semaphore_signal(barrier, inc=1, device_id={"row": lax.rem(me + step, rows_n)},
                            device_id_type=pl.DeviceIdType.MESH)

    @pl.when(here > 0)
    def _():
        pl.semaphore_signal(barrier, inc=1, device_id={"col": here - 1}, device_id_type=pl.DeviceIdType.MESH)

    @pl.when(here < parts - 1)
    def _():
        pl.semaphore_signal(barrier, inc=1, device_id={"col": here + 1}, device_id_type=pl.DeviceIdType.MESH)

    beside = jnp.where(here > 0, 1, 0) + jnp.where(here < parts - 1, 1, 0)
    pl.semaphore_wait(barrier, rows_n - 1 + beside)

    low_half = here < parts - 1 - here
    few = jnp.minimum(here, parts - 1 - here)
    order = []
    for k in range(parts - 1):
        step = jnp.where(k < 2 * few, k // 2, k - few)
        first = jnp.where(k < 2 * few, k % 2, 0) == 0
        order.append(jnp.where(first == low_half, parts - 1 - step, step))
    order.append(here)

    for q in range(parts):
        w_mine[q] = w_ref[:, q * width:(q + 1) * width]

    issued = []

    def begin(copy):
        copy.start()
        issued.append(copy)

    def send_weight(k):
        for step in range(1, rows_n):
            begin(remote(w_mine.at[order[k]], weights[k].at[pl.ds(pl.multiple_of(me * fw, fw), fw)],
                         w_send.at[k, step], w_recv.at[k, me], "row", lax.rem(me + step, rows_n)))

    send_weight(0)
    for step in range(1, rows_n):
        to = lax.rem(me + step, rows_n)
        begin(remote(f_ref.at[:, pl.ds(pl.multiple_of(to * block, block), block)],
                     ft.at[pl.ds(pl.multiple_of(me * fw, fw), fw)],
                     f_send.at[step], f_recv.at[me], "row", to))
    for k in range(1, EARLY):
        send_weight(k)

    mine = pl.ds(pl.multiple_of(me * fw, fw), fw)
    ft[mine, :] = f_ref[:, pl.ds(pl.multiple_of(me * block, block), block)]
    for k in range(parts):
        weights[k][mine, :] = w_mine[order[k]]

    tiles_ref[maxt] = jnp.zeros((tile, tile), tiles_ref.dtype)
    runs[bunches] = jnp.zeros((tile, width), runs.dtype)

    def weight_in(k):
        for step in range(1, rows_n):
            at = lax.rem(me + step, rows_n)
            place = weights[k].at[pl.ds(pl.multiple_of(at * fw, fw), fw)]
            remote(place, place, w_send.at[k, step], w_recv.at[k, at], "row", at).wait_recv()

    for step in range(1, rows_n):
        at = lax.rem(me + step, rows_n)
        place = ft.at[pl.ds(pl.multiple_of(at * fw, fw), fw)]
        remote(place, place, f_send.at[step], f_recv.at[at], "row", at).wait_recv()
    strip = min(block, 512)
    for low in range(0, feat, tile):
        for at in range(0, block, strip):
            xs[at:at + strip, low:low + tile] = ft[low:low + tile, at:at + strip].T

    def spot(k, at):
        return panels[k].at[pl.ds(at * deep, deep)]

    def share(k):
        weight_in(k)
        product = jnp.dot(xs[...], weights[k][...], preferred_element_type=jnp.float32)
        panels[k][pl.ds(me * deep, deep)] = product.astype(panels[k].dtype).reshape(deep, tile, width)
        for step in range(1, twins):
            begin(remote(spot(k, me), spot(k, me), h_send.at[k, step], h_recv.at[k, me], "row",
                         lax.rem(me + 2 * step, rows_n)))
        begin(remote(spot(k, me), spot(k, me), h_send.at[k, 0], h_recv.at[k, me], "row", sibling))

    for k in range(EARLY):
        share(k)
    for k in range(EARLY, parts):
        send_weight(k)
    fetch.wait()

    def collect(k):
        for step in range(1, twins):
            at = lax.rem(me + 2 * step, rows_n)
            remote(spot(k, at), spot(k, at), sib_send.at[k, step], h_recv.at[k, at], "row", sibling).wait_recv()
            begin(remote(spot(k, at), spot(k, at), sib_send.at[k, step], h_recv.at[k, at], "row", sibling))
        for step in range(twins):
            at = lax.rem(sibling + 2 * step, rows_n)
            remote(spot(k, at), spot(k, at), sib_send.at[k, step], h_recv.at[k, at], "row", sibling).wait_recv()

    def multiply(k):
        panel = panels[k]

        def bunch(i, total):
            left, right = [], []
            for j in range(BUNCH):
                at = i * BUNCH + j
                left.append(tiles_ref[slots_ref[at]])
                right.append(panel[cols_ref[at]])
            here_sum = jnp.dot(jnp.concatenate(left, axis=1), jnp.concatenate(right, axis=0),
                               preferred_element_type=jnp.float32)
            total = total * keep_ref[i] + here_sum
            runs[i] = total.astype(runs.dtype)
            return total

        lax.fori_loop(0, bunches, bunch, jnp.zeros((tile, width), jnp.float32))
        for row in range(trow):
            partial[k, row * tile:(row + 1) * tile, :] = runs[last_ref[row]]

    thick = rows // PIECES

    def piece(ref, which, p):
        return ref.at[which, pl.ds(p * thick, thick)]

    def stream(k):
        q = order[k]
        up = q > here
        inner = (here > 0) & (here < parts - 1)
        to = jnp.where(up, here + 1, here - 1)
        slot = jnp.where(q == here - 1, parts, q)
        for p in range(PIECES):
            @pl.when(inner)
            def _():
                remote(piece(landed, q, p), piece(landed, q, p), z_send.at[k, p], z_recv.at[q, p],
                       "col", to).wait_recv()
                partial[k, p * thick:(p + 1) * thick, :] = (
                    partial[k, p * thick:(p + 1) * thick, :].astype(jnp.float32)
                    + landed[q, p * thick:(p + 1) * thick, :].astype(jnp.float32)).astype(partial.dtype)

            begin(remote(piece(partial, k, p), piece(landed, slot, p), z_send.at[k, p], z_recv.at[slot, p],
                         "col", to))

    for k in range(parts - 1):
        collect(k)
        multiply(k)
        stream(k)
        if k == 0:
            for later in range(EARLY, parts):
                share(later)
    own = parts - 1
    collect(own)
    multiply(own)
    for p in range(PIECES):
        span = slice(p * thick, (p + 1) * thick)
        for side, slot, there in ((0, here, here > 0), (1, parts, here < parts - 1)):
            @pl.when(there)
            def _():
                remote(piece(landed, slot, p), piece(landed, slot, p), z_send.at[own, p], z_recv.at[slot, p],
                       "col", here).wait_recv()

        total = partial[own, span, :].astype(jnp.float32)
        total = total + jnp.where(here > 0, landed[here, span, :].astype(jnp.float32), 0.0)
        total = total + jnp.where(here < parts - 1, landed[parts, span, :].astype(jnp.float32), 0.0)
        out_ref[span, :] = total.astype(out_ref.dtype)
    for copy in issued:
        copy.wait_send()


def layer(lists, features, weight_t, tiles, rows_n, parts):
    maxt, tile, _ = tiles.shape
    fw, nodes = features.shape
    outs = weight_t.shape[1]
    width = outs // parts
    feat = fw * rows_n
    block = nodes // rows_n
    trow = lists[3].shape[0]
    rows = trow * tile
    bunches = lists[2].shape[0] - 1
    kind = features.dtype
    smem = pl.BlockSpec(memory_space=pltpu.SMEM)
    vmem = pl.BlockSpec(memory_space=pltpu.VMEM)
    dma = pltpu.SemaphoreType.DMA
    return pl.pallas_call(
        functools.partial(layer_kernel, rows_n, parts),
        out_shape=jax.ShapeDtypeStruct((rows, width), kind),
        in_specs=[smem] * 4 + [vmem, vmem, pl.BlockSpec(memory_space=pl.ANY)],
        out_specs=vmem,
        scratch_shapes=[
            pltpu.VMEM((maxt + 1, tile, tile), kind),
            pltpu.VMEM((feat, block), kind),
            pltpu.VMEM((block, feat), kind),
            pltpu.VMEM((parts, fw, width), kind),
            [pltpu.VMEM((feat, width), kind) for _ in range(parts)],
            [pltpu.VMEM((nodes // tile, tile, width), kind) for _ in range(parts)],
            pltpu.VMEM((bunches + 1, tile, width), kind),
            pltpu.VMEM((parts, rows, width), kind),
            pltpu.VMEM((parts + 1, rows, width), kind),
            dma,
            dma((rows_n,)),
            dma((rows_n,)),
            dma((parts, rows_n)),
            dma((parts, rows_n)),
            dma((parts, rows_n)),
            dma((parts, rows_n)),
            dma((parts, rows_n)),
            dma((parts, PIECES)),
            dma((parts + 1, PIECES)),
        ],
        compiler_params=pltpu.CompilerParams(
            collective_id=0, has_side_effects=True, vmem_limit_bytes=VMEM_LIMIT
        ),
        name="layer",
    )(*lists, features, weight_t, tiles)


def solution(mesh):
    placed = (
        P("col", "row"),
        P(None, "row"),
        P(("row", "col"), None, None),
        P(None, ("row", "col")),
        P(("row", "col")),
    )
    rows_n = mesh.shape["row"]
    parts = mesh.shape["col"]

    def body(features, weight_t, tiles, coords, counts):
        maxt, tile, _ = tiles.shape
        trow = features.shape[0] * parts // rows_n // tile
        bunches = (maxt + trow * (BUNCH - 1)) // BUNCH
        lists = plan(coords, counts, trow, bunches)
        return layer(lists, features.T, weight_t.T, tiles, rows_n, parts)

    return jax.shard_map(
        body, mesh=mesh, in_specs=placed, out_specs=P("row", "col"), check_vma=False
    )
```

```python
import functools

import jax
import jax.numpy as jnp
from jax import lax
from jax.experimental import pallas as pl
from jax.experimental.pallas import tpu as pltpu
from jax.sharding import PartitionSpec as P

BUNCH = 2
UNROLL = 16
PIECES = 4
EARLY = 2
HALF = 64
VMEM_LIMIT = 62 * 1024 * 1024


def remote(src, dst, send, recv, axis, to):
    return pltpu.make_async_remote_copy(
        src_ref=src,
        dst_ref=dst,
        send_sem=send,
        recv_sem=recv,
        device_id={axis: to},
        device_id_type=pl.DeviceIdType.MESH,
    )


def plan(coords_ref, count, trow, lists_ref, keep_ref):
    maxt = coords_ref.shape[1]
    spots = lists_ref.shape[1]
    bunches = maxt // BUNCH + trow * (BUNCH - 1) // BUNCH
    lists_ref[...] = jnp.zeros(lists_ref.shape, jnp.int32)
    keep_ref[...] = jnp.zeros(keep_ref.shape, jnp.float32)

    def iota(shape, axis):
        return lax.broadcasted_iota(jnp.int32, shape, axis)

    def total(mask, value, axis):
        return jnp.sum(jnp.where(mask, value, 0), axis=axis, keepdims=True, dtype=jnp.int32)

    slot = iota((1, maxt), 1)
    row = jnp.where(slot < count, coords_ref[0:1, :], 2 * trow)
    square = jnp.broadcast_to(row, (maxt, maxt))
    turned = square.T
    rank = total((square == turned) & (iota((maxt, maxt), 0) < iota((maxt, maxt), 1)), 1, 0)

    def rounds(number):
        return (number + (BUNCH - 1)) // BUNCH

    match = iota((trow, maxt), 0) == row
    need_down = rounds(total(match, 1, 1))
    spot = iota((maxt, 128), 1)
    need_along = rounds(total(turned[:, :128] == spot, 1, 0))
    down = iota((trow, 128), 0)
    along = iota((trow, 128), 1)
    base_down = total(along < down, need_along, 1)
    base_along = total(down < along, need_down, 0)
    last = jnp.where(need_along > 0, base_along + need_along - 1, bunches)
    place = jnp.where(slot < count, rank + total(match, base_down * BUNCH, 0), -1)
    place_down = jnp.broadcast_to(place, (maxt, maxt)).T[:, :128]
    col_down = jnp.broadcast_to(coords_ref[1:2, :], (maxt, maxt)).T[:, :128]
    for low in range(0, spots, 128):
        hit = place_down == spot + low
        lists_ref[0:1, low:low + 128] = total(hit, iota((maxt, 128), 0) - maxt, 0) + maxt
        lists_ref[1:2, low:low + 128] = total(hit, col_down, 0)
        begins = total((base_down == along + low) & (need_down > 0), 1, 0)
        keep_ref[0:1, low:low + 128] = 1.0 - begins.astype(jnp.float32)
    lists_ref[2:3, 0:128] = jnp.where(slot[:, :128] < trow, last, 0)


def layer_kernel(rows_n, parts, count_ref, coords_ref, f_ref, w_ref, tiles_hbm, out_ref,
                 tiles_ref, ft, xs, w_mine, weights, panels, spread, runs, partial, landed,
                 lists_made, keep_made, lists_ref, keep_ref,
                 local_sem, f_send, f_recv, w_send, w_recv, h_send, h_recv, sib_send, z_send, z_recv):
    me = lax.axis_index("row")
    here = lax.axis_index("col")
    maxt, tile, _ = tiles_hbm.shape
    fw, nodes = f_ref.shape
    block = nodes // rows_n
    deep = block // tile // 2
    rows, width = out_ref.shape
    split = width // HALF
    chunks = parts * split
    feat = rows_n * fw
    bunches = runs.shape[0] - 1
    trow = rows // tile
    core = me % 2
    sibling = me + 1 - 2 * core
    twins = rows_n // 2

    fetch = pltpu.make_async_copy(tiles_hbm, tiles_ref.at[pl.ds(0, maxt)], local_sem.at[0])
    fetch.start()

    barrier = pltpu.get_barrier_semaphore()
    for step in range(1, rows_n):
        pl.semaphore_signal(barrier, inc=1, device_id={"row": lax.rem(me + step, rows_n)},
                            device_id_type=pl.DeviceIdType.MESH)

    @pl.when(here > 0)
    def _():
        pl.semaphore_signal(barrier, inc=1, device_id={"col": here - 1}, device_id_type=pl.DeviceIdType.MESH)

    @pl.when(here < parts - 1)
    def _():
        pl.semaphore_signal(barrier, inc=1, device_id={"col": here + 1}, device_id_type=pl.DeviceIdType.MESH)

    beside = jnp.where(here > 0, 1, 0) + jnp.where(here < parts - 1, 1, 0)
    pl.semaphore_wait(barrier, rows_n - 1 + beside)

    low_half = here < parts - 1 - here
    few = jnp.minimum(here, parts - 1 - here)
    order = []
    for k in range(parts - 1):
        step = jnp.where(k < 2 * few, k // 2, k - few)
        first = jnp.where(k < 2 * few, k % 2, 0) == 0
        order.append(jnp.where(first == low_half, parts - 1 - step, step))
    order.append(here)

    for q in range(parts):
        w_mine[q] = w_ref[:, q * width:(q + 1) * width]

    issued = []

    def begin(copy):
        copy.start()
        issued.append(copy)

    def send_weight(k):
        for step in range(1, rows_n):
            begin(remote(w_mine.at[order[k]], weights[k].at[pl.ds(pl.multiple_of(me * fw, fw), fw)],
                         w_send.at[k, step], w_recv.at[k, me], "row", lax.rem(me + step, rows_n)))

    send_weight(0)
    for step in range(1, rows_n):
        to = lax.rem(me + step, rows_n)
        begin(remote(f_ref.at[:, pl.ds(pl.multiple_of(to * block, block), block)],
                     ft.at[pl.ds(pl.multiple_of(me * fw, fw), fw)],
                     f_send.at[step], f_recv.at[me], "row", to))
    for k in range(1, EARLY):
        send_weight(k)

    mine = pl.ds(pl.multiple_of(me * fw, fw), fw)
    ft[mine, :] = f_ref[:, pl.ds(pl.multiple_of(me * block, block), block)]
    for k in range(parts):
        weights[k][mine, :] = w_mine[order[k]]

    tiles_ref[maxt] = jnp.zeros((tile, tile), tiles_ref.dtype)
    runs[bunches] = jnp.zeros((tile, tile), runs.dtype)
    plan(coords_ref, count_ref[0], trow, lists_made, keep_made)
    moves = [
        pltpu.make_async_copy(lists_made, lists_ref, local_sem.at[1]),
        pltpu.make_async_copy(keep_made, keep_ref, local_sem.at[2]),
    ]
    for move in moves:
        move.start()

    def weight_in(k):
        for step in range(1, rows_n):
            at = lax.rem(me + step, rows_n)
            place = weights[k].at[pl.ds(pl.multiple_of(at * fw, fw), fw)]
            remote(place, place, w_send.at[k, step], w_recv.at[k, at], "row", at).wait_recv()

    for step in range(1, rows_n):
        at = lax.rem(me + step, rows_n)
        place = ft.at[pl.ds(pl.multiple_of(at * fw, fw), fw)]
        remote(place, place, f_send.at[step], f_recv.at[at], "row", at).wait_recv()
    strip = min(block, 512)
    for low in range(0, feat, tile):
        for at in range(0, block, strip):
            xs[at:at + strip, low:low + tile] = ft[low:low + tile, at:at + strip].T

    def spot(c, at):
        return panels[c].at[pl.ds(at * deep, deep)]

    def share(k):
        weight_in(k)
        product = jnp.dot(xs[...], weights[k][...], preferred_element_type=jnp.float32).astype(xs.dtype)
        for h in range(split):
            c = k * split + h
            cut = product[:, h * HALF:(h + 1) * HALF]
            packed = jnp.concatenate([cut[:block // 2], cut[block // 2:]], axis=1)
            panels[c][pl.ds(me * deep, deep)] = packed.reshape(deep, tile, tile)
            for step in range(1, twins):
                begin(remote(spot(c, me), spot(c, me), h_send.at[c, step], h_recv.at[c, me], "row",
                             lax.rem(me + 2 * step, rows_n)))
            begin(remote(spot(c, me), spot(c, me), h_send.at[c, 0], h_recv.at[c, me], "row", sibling))

    for k in range(EARLY):
        share(k)
    for k in range(EARLY, parts):
        send_weight(k)
    fetch.wait()
    for move in moves:
        move.wait()

    def collect(c):
        for step in range(1, twins):
            at = lax.rem(me + 2 * step, rows_n)
            passed = remote(spot(c, at), spot(c, at), sib_send.at[c, step], h_recv.at[c, at], "row", sibling)
            passed.wait_recv()
            begin(passed)
        for step in range(twins):
            at = lax.rem(sibling + 2 * step, rows_n)
            remote(spot(c, at), spot(c, at), sib_send.at[c, step], h_recv.at[c, at], "row", sibling).wait_recv()

    def multiply(c):
        for at in range(rows_n * deep):
            both = panels[c][at]
            low = at // deep * 2 * deep + at % deep
            spread[low] = both
            spread[low + deep] = jnp.concatenate([both[:, HALF:], both[:, :HALF]], axis=1)

        def bunch(i, total):
            left, right = [], []
            for j in range(BUNCH):
                at = i * BUNCH + j
                left.append(tiles_ref[lists_ref[0, at]])
                right.append(spread[lists_ref[1, at]])
            part = jnp.dot(jnp.concatenate(left, axis=1), jnp.concatenate(right, axis=0),
                           preferred_element_type=jnp.float32)
            total = total * keep_ref[0, i] + part
            runs[i] = total.astype(runs.dtype)
            return total

        lax.fori_loop(0, bunches, bunch, jnp.zeros((tile, tile), jnp.float32), unroll=UNROLL)
        for row in range(trow // 2):
            low = runs[lists_ref[2, row]]
            high = runs[lists_ref[2, row + trow // 2]]
            partial[c, row * tile:(row + 1) * tile, :] = jnp.concatenate([low[:, :HALF], high[:, :HALF]], axis=1)

    thick = rows // 2 // PIECES

    def piece(ref, which, p):
        return ref.at[which, pl.ds(p * thick, thick)]

    def stream(c):
        q = order[c // split]
        up = q > here
        inner = (here > 0) & (here < parts - 1)
        to = jnp.where(up, here + 1, here - 1)
        came = q * split + c % split
        goes = jnp.where(q == here - 1, parts, q) * split + c % split
        for p in range(PIECES):
            span = slice(p * thick, (p + 1) * thick)

            @pl.when(inner)
            def _():
                remote(piece(landed, came, p), piece(landed, came, p), z_send.at[c, p], z_recv.at[came, p],
                       "col", to).wait_recv()
                partial[c, span, :] = (partial[c, span, :].astype(jnp.float32)
                                       + landed[came, span, :].astype(jnp.float32)).astype(partial.dtype)

            begin(remote(piece(partial, c, p), piece(landed, goes, p), z_send.at[c, p], z_recv.at[goes, p],
                         "col", to))

    for c in range(chunks - split):
        collect(c)
        multiply(c)
        stream(c)
        if c == 0:
            for later in range(EARLY, parts):
                share(later)
    for h in range(split):
        c = chunks - split + h
        collect(c)
        multiply(c)
    for p in range(PIECES):
        for h in range(split):
            span = slice(p * thick, (p + 1) * thick)
            c = chunks - split + h
            below = here * split + h
            above = parts * split + h
            for slot, there in ((below, here > 0), (above, here < parts - 1)):
                @pl.when(there)
                def _():
                    remote(piece(landed, slot, p), piece(landed, slot, p), z_send.at[c, p], z_recv.at[slot, p],
                           "col", here).wait_recv()

            total = partial[c, span, :].astype(jnp.float32)
            total = total + jnp.where(here > 0, landed[below, span, :].astype(jnp.float32), 0.0)
            total = total + jnp.where(here < parts - 1, landed[above, span, :].astype(jnp.float32), 0.0)
            total = total.astype(out_ref.dtype)
            high = slice(rows // 2 + p * thick, rows // 2 + (p + 1) * thick)
            out_ref[span, h * HALF:(h + 1) * HALF] = total[:, :HALF]
            out_ref[high, h * HALF:(h + 1) * HALF] = total[:, HALF:]
    for copy in issued:
        copy.wait_send()


def layer(features, weight_t, tiles, coords, counts, rows_n, parts):
    maxt, tile, _ = tiles.shape
    fw, nodes = features.shape
    outs = weight_t.shape[1]
    width = outs // parts
    feat = fw * rows_n
    block = nodes // rows_n
    rows = nodes * parts // rows_n
    trow = rows // tile
    bunches = maxt // BUNCH + trow * (BUNCH - 1) // BUNCH
    spots = -(-bunches * BUNCH // 128) * 128
    chunks = outs // HALF
    split = width // HALF
    kind = features.dtype
    smem = pl.BlockSpec(memory_space=pltpu.SMEM)
    vmem = pl.BlockSpec(memory_space=pltpu.VMEM)
    dma = pltpu.SemaphoreType.DMA
    return pl.pallas_call(
        functools.partial(layer_kernel, rows_n, parts),
        out_shape=jax.ShapeDtypeStruct((rows, width), kind),
        in_specs=[smem, vmem, vmem, vmem, pl.BlockSpec(memory_space=pl.ANY)],
        out_specs=vmem,
        scratch_shapes=[
            pltpu.VMEM((maxt + 1, tile, tile), kind),
            pltpu.VMEM((feat, block), kind),
            pltpu.VMEM((block, feat), kind),
            pltpu.VMEM((parts, fw, width), kind),
            [pltpu.VMEM((feat, width), kind) for _ in range(parts)],
            [pltpu.VMEM((nodes // tile // 2, tile, tile), kind) for _ in range(chunks)],
            pltpu.VMEM((nodes // tile, tile, tile), kind),
            pltpu.VMEM((bunches + 1, tile, tile), kind),
            pltpu.VMEM((chunks, rows // 2, tile), kind),
            pltpu.VMEM((chunks + split, rows // 2, tile), kind),
            pltpu.VMEM((8, spots), jnp.int32),
            pltpu.VMEM((8, spots), jnp.float32),
            pltpu.SMEM((8, spots), jnp.int32),
            pltpu.SMEM((8, spots), jnp.float32),
            dma((3,)),
            dma((rows_n,)),
            dma((rows_n,)),
            dma((parts, rows_n)),
            dma((parts, rows_n)),
            dma((chunks, rows_n)),
            dma((chunks, rows_n)),
            dma((chunks, rows_n)),
            dma((chunks, PIECES)),
            dma((chunks + split, PIECES)),
        ],
        compiler_params=pltpu.CompilerParams(
            collective_id=0, has_side_effects=True, vmem_limit_bytes=VMEM_LIMIT
        ),
        name="layer",
    )(counts, coords, features, weight_t, tiles)


def solution(mesh):
    placed = (
        P("col", "row"),
        P(None, "row"),
        P(("row", "col"), None, None),
        P(None, ("row", "col")),
        P(("row", "col")),
    )
    rows_n = mesh.shape["row"]
    parts = mesh.shape["col"]

    def body(features, weight_t, tiles, coords, counts):
        return layer(features.T, weight_t.T, tiles, coords, counts, rows_n, parts)

    return jax.shard_map(
        body, mesh=mesh, in_specs=placed, out_specs=P("row", "col"), check_vma=False
    )
```

```python
import functools

import jax
import jax.numpy as jnp
from jax import lax
from jax.experimental import pallas as pl
from jax.experimental.pallas import tpu as pltpu
from jax.sharding import PartitionSpec as P

BUNCH = 2
UNROLL = 36
PIECES = 4
HALF = 64
VMEM_LIMIT = 62 * 1024 * 1024


def remote(src, dst, send, recv, axis, to):
    return pltpu.make_async_remote_copy(
        src_ref=src,
        dst_ref=dst,
        send_sem=send,
        recv_sem=recv,
        device_id={axis: to},
        device_id_type=pl.DeviceIdType.MESH,
    )


def plan(coords_ref, count, trow, lists_ref, keep_ref):
    maxt = coords_ref.shape[1]
    spots = lists_ref.shape[1]
    bunches = maxt // BUNCH + trow * (BUNCH - 1) // BUNCH
    lists_ref[...] = jnp.zeros(lists_ref.shape, jnp.int32)
    keep_ref[...] = jnp.zeros(keep_ref.shape, jnp.float32)

    def iota(shape, axis):
        return lax.broadcasted_iota(jnp.int32, shape, axis)

    def total(mask, value, axis):
        return jnp.sum(jnp.where(mask, value, 0), axis=axis, keepdims=True, dtype=jnp.int32)

    slot = iota((1, maxt), 1)
    row = jnp.where(slot < count, coords_ref[0:1, :], 2 * trow)
    square = jnp.broadcast_to(row, (maxt, maxt))
    turned = square.T
    rank = total((square == turned) & (iota((maxt, maxt), 0) < iota((maxt, maxt), 1)), 1, 0)

    def rounds(number):
        return (number + (BUNCH - 1)) // BUNCH

    match = iota((trow, maxt), 0) == row
    need_down = rounds(total(match, 1, 1))
    spot = iota((maxt, 128), 1)
    need_along = rounds(total(turned[:, :128] == spot, 1, 0))
    down = iota((trow, 128), 0)
    along = iota((trow, 128), 1)
    base_down = total(along < down, need_along, 1)
    base_along = total(down < along, need_down, 0)
    last = jnp.where(need_along > 0, base_along + need_along - 1, bunches)
    place = jnp.where(slot < count, rank + total(match, base_down * BUNCH, 0), -1)
    place_down = jnp.broadcast_to(place, (maxt, maxt)).T[:, :128]
    col_down = jnp.broadcast_to(coords_ref[1:2, :], (maxt, maxt)).T[:, :128]
    for low in range(0, spots, 128):
        hit = place_down == spot + low
        lists_ref[0:1, low:low + 128] = total(hit, iota((maxt, 128), 0) - maxt, 0) + maxt
        lists_ref[1:2, low:low + 128] = total(hit, col_down, 0)
        begins = total((base_down == along + low) & (need_down > 0), 1, 0)
        keep_ref[0:1, low:low + 128] = 1.0 - begins.astype(jnp.float32)
    lists_ref[2:3, 0:128] = jnp.where(slot[:, :128] < trow, last, 0)


def layer_kernel(rows_n, parts, count_ref, coords_ref, f_ref, w_ref, tiles_hbm, out_ref,
                 tiles_ref, ft, xs, w_mine, weights, panels, spread, runs, partial, landed,
                 lists_made, keep_made, lists_ref, keep_ref,
                 local_sem, f_send, f_recv, w_send, w_recv, h_send, h_recv, sib_send, z_send, z_recv):
    me = lax.axis_index("row")
    here = lax.axis_index("col")
    maxt, tile, _ = tiles_hbm.shape
    fw, nodes = f_ref.shape
    block = nodes // rows_n
    half = block // 2
    deep = block // tile // 4
    rows, width = out_ref.shape
    split = width // HALF
    chunks = parts * split
    feat = rows_n * fw
    bunches = runs.shape[0] - 1
    trow = rows // tile
    core = me % 2
    sibling = me + 1 - 2 * core
    twins = rows_n // 2

    fetch = pltpu.make_async_copy(tiles_hbm, tiles_ref.at[pl.ds(0, maxt)], local_sem.at[0])
    fetch.start()

    barrier = pltpu.get_barrier_semaphore()
    for step in range(1, rows_n):
        pl.semaphore_signal(barrier, inc=1, device_id={"row": lax.rem(me + step, rows_n)},
                            device_id_type=pl.DeviceIdType.MESH)

    @pl.when(here > 0)
    def _():
        pl.semaphore_signal(barrier, inc=1, device_id={"col": here - 1}, device_id_type=pl.DeviceIdType.MESH)

    @pl.when(here < parts - 1)
    def _():
        pl.semaphore_signal(barrier, inc=1, device_id={"col": here + 1}, device_id_type=pl.DeviceIdType.MESH)

    beside = jnp.where(here > 0, 1, 0) + jnp.where(here < parts - 1, 1, 0)
    pl.semaphore_wait(barrier, rows_n - 1 + beside)

    low_half = here < parts - 1 - here
    few = jnp.minimum(here, parts - 1 - here)

    def target(k):
        paired = k < 2 * few
        step = jnp.where(paired, k // 2, k - few)
        first = jnp.where(paired, k % 2, 0) == 0
        return jnp.where(k == parts - 1, here, jnp.where(first == low_half, parts - 1 - step, step))

    for q in range(parts):
        w_mine[q] = w_ref[:, q * width:(q + 1) * width]

    issued = []

    def begin(copy):
        copy.start()
        issued.append(copy)

    def send_weight(k):
        for step in range(1, rows_n):
            begin(remote(w_mine.at[target(k)], weights[k].at[pl.ds(pl.multiple_of(me * fw, fw), fw)],
                         w_send.at[k, step], w_recv.at[k, me], "row", lax.rem(me + step, rows_n)))

    send_weight(0)
    for part in range(2):
        for step in range(1, rows_n):
            to = lax.rem(me + step, rows_n)
            begin(remote(f_ref.at[:, pl.ds(pl.multiple_of(to * block + part * half, half), half)],
                         ft.at[part, pl.ds(pl.multiple_of(me * fw, fw), fw)],
                         f_send.at[part, step], f_recv.at[part, me], "row", to))

    mine = pl.ds(pl.multiple_of(me * fw, fw), fw)
    for part in range(2):
        ft[part, mine, :] = f_ref[:, pl.ds(pl.multiple_of(me * block + part * half, half), half)]
    for k in range(parts):
        weights[k][mine, :] = w_mine[target(k)]

    tiles_ref[maxt] = jnp.zeros((tile, tile), tiles_ref.dtype)
    runs[bunches] = jnp.zeros((tile, tile), runs.dtype)
    plan(coords_ref, count_ref[0], trow, lists_made, keep_made)
    moves = [
        pltpu.make_async_copy(lists_made, lists_ref, local_sem.at[1]),
        pltpu.make_async_copy(keep_made, keep_ref, local_sem.at[2]),
    ]
    for move in moves:
        move.start()

    def weight_in(k):
        for step in range(1, rows_n):
            at = lax.rem(me + step, rows_n)
            place = weights[k].at[pl.ds(pl.multiple_of(at * fw, fw), fw)]
            remote(place, place, w_send.at[k, step], w_recv.at[k, at], "row", at).wait_recv()

    group = tile // fw
    groups = rows_n // group
    strip = min(half, 512)

    def turn_in(part):
        for turn in range(groups):
            low = lax.rem(me // group + turn, groups) * group
            for j in range(group):
                at = low + j
                place = ft.at[part, pl.ds(pl.multiple_of(at * fw, fw), fw)]

                @pl.when(at != me)
                def _():
                    remote(place, place, f_send.at[part, 0], f_recv.at[part, at], "row", me).wait_recv()

            lane = pl.ds(pl.multiple_of(low * fw, tile), tile)
            for at in range(0, half, strip):
                xs[part * half + at:part * half + at + strip, lane] = ft[part, lane, at:at + strip].T

    def spot(c, at, part):
        if part is None:
            return panels.at[c, pl.ds(at * 2 * deep, 2 * deep)]
        return panels.at[c, pl.ds((at * 2 + part) * deep, deep)]

    def row_of(c, part):
        return chunks if part == 1 else c

    def send_chunk(c, part):
        place, line = spot(c, me, part), row_of(c, part)
        for step in range(1, twins):
            begin(remote(place, place, h_send.at[line, step], h_recv.at[line, me], "row",
                         lax.rem(me + 2 * step, rows_n)))
        begin(remote(place, place, h_send.at[line, 0], h_recv.at[line, me], "row", sibling))

    def make(k, part):
        product = jnp.dot(xs[part * half:(part + 1) * half, :], weights[k][...],
                          preferred_element_type=jnp.float32).astype(xs.dtype)
        for h in range(split):
            cut = product[:, h * HALF:(h + 1) * HALF]
            packed = jnp.concatenate([cut[:half // 2], cut[half // 2:]], axis=1)
            panels[k * split + h, pl.ds((me * 2 + part) * deep, deep)] = packed.reshape(deep, tile, tile)

    def forward(c, at, step, part):
        place, line = spot(c, at, part), row_of(c, part)
        return remote(place, place, sib_send.at[line, step], h_recv.at[line, at], "row", sibling)

    def collect(c, sections):
        for part in sections:
            for step in range(1, twins):
                passed = forward(c, lax.rem(me + 2 * step, rows_n), step, part)
                passed.wait_recv()
                passed.start()
        for part in sections:
            for step in range(twins):
                forward(c, lax.rem(sibling + 2 * step, rows_n), step, part).wait_recv()

    def multiply(c):
        for at in range(rows_n * 2 * deep):
            both = panels[c, at]
            low = at // deep * 2 * deep + at % deep
            spread[low] = both
            spread[low + deep] = jnp.concatenate([both[:, HALF:], both[:, :HALF]], axis=1)

        def bunch(i, total):
            left, right = [], []
            for j in range(BUNCH):
                at = i * BUNCH + j
                left.append(tiles_ref[lists_ref[0, at]])
                right.append(spread[lists_ref[1, at]])
            part = jnp.dot(jnp.concatenate(left, axis=1), jnp.concatenate(right, axis=0),
                           preferred_element_type=jnp.float32)
            total = total * keep_ref[0, i] + part
            runs[i] = total.astype(runs.dtype)
            return total

        lax.fori_loop(0, bunches, bunch, jnp.zeros((tile, tile), jnp.float32), unroll=UNROLL)
        for row in range(trow // 2):
            low = runs[lists_ref[2, row]]
            high = runs[lists_ref[2, row + trow // 2]]
            partial[c, row * tile:(row + 1) * tile, :] = jnp.concatenate([low[:, :HALF], high[:, :HALF]], axis=1)

    thick = rows // 2 // PIECES

    def piece(ref, which, p):
        return ref.at[which, pl.ds(p * thick, thick)]

    def outgoing(c, p):
        q = target(c // split)
        to = jnp.where(q > here, here + 1, here - 1)
        goes = jnp.where(q == here - 1, parts, q) * split + c % split
        return remote(piece(partial, c, p), piece(landed, goes, p), z_send.at[c, p], z_recv.at[goes, p],
                      "col", to)

    def stream(c):
        came = target(c // split) * split + c % split
        for p in range(PIECES):
            @pl.when((here > 0) & (here < parts - 1))
            def _():
                span = slice(p * thick, (p + 1) * thick)
                place = piece(landed, came, p)
                remote(place, place, z_send.at[c, p], z_recv.at[came, p], "col", here).wait_recv()
                partial[c, span, :] = (partial[c, span, :].astype(jnp.float32)
                                       + landed[came, span, :].astype(jnp.float32)).astype(partial.dtype)

            outgoing(c, p).start()

    for part in range(2):
        turn_in(part)
        if part == 0:
            weight_in(0)
        make(0, part)
        send_chunk(0, part)
    for h in range(1, split):
        send_chunk(h, None)
    for k in range(1, parts):
        send_weight(k)
    fetch.wait()
    for move in moves:
        move.wait()
    collect(0, (0, 1))
    multiply(0)
    stream(0)
    for k in range(1, parts):
        weight_in(k)
        for part in range(2):
            make(k, part)
        for h in range(split):
            send_chunk(k * split + h, None)

    def phase(c, carry):
        collect(c, (None,))
        multiply(c)

        @pl.when(c < chunks - split)
        def _():
            stream(c)

        return carry

    lax.fori_loop(1, chunks, phase, 0)
    for p in range(PIECES):
        for h in range(split):
            span = slice(p * thick, (p + 1) * thick)
            c = chunks - split + h
            below = here * split + h
            above = parts * split + h
            for slot, there in ((below, here > 0), (above, here < parts - 1)):
                @pl.when(there)
                def _():
                    remote(piece(landed, slot, p), piece(landed, slot, p), z_send.at[c, p], z_recv.at[slot, p],
                           "col", here).wait_recv()

            total = partial[c, span, :].astype(jnp.float32)
            total = total + jnp.where(here > 0, landed[below, span, :].astype(jnp.float32), 0.0)
            total = total + jnp.where(here < parts - 1, landed[above, span, :].astype(jnp.float32), 0.0)
            total = total.astype(out_ref.dtype)
            high = slice(rows // 2 + p * thick, rows // 2 + (p + 1) * thick)
            out_ref[span, h * HALF:(h + 1) * HALF] = total[:, :HALF]
            out_ref[high, h * HALF:(h + 1) * HALF] = total[:, HALF:]
    for copy in issued:
        copy.wait_send()
    for part in range(2):
        for step in range(1, twins):
            forward(0, lax.rem(me + 2 * step, rows_n), step, part).wait_send()

    def settle(c, carry):
        for step in range(1, twins):
            forward(c, lax.rem(me + 2 * step, rows_n), step, None).wait_send()
        return carry

    lax.fori_loop(1, chunks, settle, 0)

    def drain(c, carry):
        for p in range(PIECES):
            outgoing(c, p).wait_send()
        return carry

    lax.fori_loop(0, chunks - split, drain, 0)


def layer(features, weight_t, tiles, coords, counts, rows_n, parts):
    maxt, tile, _ = tiles.shape
    fw, nodes = features.shape
    outs = weight_t.shape[1]
    width = outs // parts
    feat = fw * rows_n
    block = nodes // rows_n
    rows = nodes * parts // rows_n
    trow = rows // tile
    bunches = maxt // BUNCH + trow * (BUNCH - 1) // BUNCH
    spots = -(-bunches * BUNCH // 128) * 128
    chunks = outs // HALF
    split = width // HALF
    kind = features.dtype
    smem = pl.BlockSpec(memory_space=pltpu.SMEM)
    vmem = pl.BlockSpec(memory_space=pltpu.VMEM)
    dma = pltpu.SemaphoreType.DMA
    return pl.pallas_call(
        functools.partial(layer_kernel, rows_n, parts),
        out_shape=jax.ShapeDtypeStruct((rows, width), kind),
        in_specs=[smem, vmem, vmem, vmem, pl.BlockSpec(memory_space=pl.ANY)],
        out_specs=vmem,
        scratch_shapes=[
            pltpu.VMEM((maxt + 1, tile, tile), kind),
            pltpu.VMEM((2, feat, block // 2), kind),
            pltpu.VMEM((block, feat), kind),
            pltpu.VMEM((parts, fw, width), kind),
            [pltpu.VMEM((feat, width), kind) for _ in range(parts)],
            pltpu.VMEM((chunks, nodes // tile // 2, tile, tile), kind),
            pltpu.VMEM((nodes // tile, tile, tile), kind),
            pltpu.VMEM((bunches + 1, tile, tile), kind),
            pltpu.VMEM((chunks, rows // 2, tile), kind),
            pltpu.VMEM((chunks + split, rows // 2, tile), kind),
            pltpu.VMEM((8, spots), jnp.int32),
            pltpu.VMEM((8, spots), jnp.float32),
            pltpu.SMEM((8, spots), jnp.int32),
            pltpu.SMEM((8, spots), jnp.float32),
            dma((3,)),
            dma((2, rows_n)),
            dma((2, rows_n)),
            dma((parts, rows_n)),
            dma((parts, rows_n)),
            dma((chunks + 1, rows_n)),
            dma((chunks + 1, rows_n)),
            dma((chunks + 1, rows_n)),
            dma((chunks, PIECES)),
            dma((chunks + split, PIECES)),
        ],
        compiler_params=pltpu.CompilerParams(
            collective_id=0, has_side_effects=True, vmem_limit_bytes=VMEM_LIMIT
        ),
        name="layer",
    )(counts, coords, features, weight_t, tiles)


def solution(mesh):
    placed = (
        P("col", "row"),
        P(None, "row"),
        P(("row", "col"), None, None),
        P(None, ("row", "col")),
        P(("row", "col")),
    )
    rows_n = mesh.shape["row"]
    parts = mesh.shape["col"]

    def body(features, weight_t, tiles, coords, counts):
        return layer(features.T, weight_t.T, tiles, coords, counts, rows_n, parts)

    return jax.shard_map(
        body, mesh=mesh, in_specs=placed, out_specs=P("row", "col"), check_vma=False
    )
```

```python
import functools

import jax
import jax.numpy as jnp
from jax import lax
from jax.experimental import pallas as pl
from jax.experimental.pallas import tpu as pltpu
from jax.sharding import PartitionSpec as P

BUNCH = 2
UNROLL = 36
CUTS = 2
PIECES = 4
HALF = 64
VMEM_LIMIT = 62 * 1024 * 1024


def remote(src, dst, send, recv, axis, to):
    return pltpu.make_async_remote_copy(
        src_ref=src,
        dst_ref=dst,
        send_sem=send,
        recv_sem=recv,
        device_id={axis: to},
        device_id_type=pl.DeviceIdType.MESH,
    )


def plan(coords_ref, count, trow, lists_ref, keep_ref):
    maxt = coords_ref.shape[1]
    spots = lists_ref.shape[1]
    bunches = maxt // BUNCH + trow * (BUNCH - 1) // BUNCH
    lists_ref[...] = jnp.zeros(lists_ref.shape, jnp.int32)
    keep_ref[...] = jnp.zeros(keep_ref.shape, jnp.float32)

    def iota(shape, axis):
        return lax.broadcasted_iota(jnp.int32, shape, axis)

    def total(mask, value, axis):
        return jnp.sum(jnp.where(mask, value, 0), axis=axis, keepdims=True, dtype=jnp.int32)

    slot = iota((1, maxt), 1)
    row = jnp.where(slot < count, coords_ref[0:1, :], 2 * trow)
    square = jnp.broadcast_to(row, (maxt, maxt))
    turned = square.T
    rank = total((square == turned) & (iota((maxt, maxt), 0) < iota((maxt, maxt), 1)), 1, 0)

    def rounds(number):
        return (number + (BUNCH - 1)) // BUNCH

    match = iota((trow, maxt), 0) == row
    need_down = rounds(total(match, 1, 1))
    spot = iota((maxt, 128), 1)
    need_along = rounds(total(turned[:, :128] == spot, 1, 0))
    down = iota((trow, 128), 0)
    along = iota((trow, 128), 1)
    base_down = total(along < down, need_along, 1)
    base_along = total(down < along, need_down, 0)
    last = jnp.where(need_along > 0, base_along + need_along - 1, bunches)
    place = jnp.where(slot < count, rank + total(match, base_down * BUNCH, 0), -1)
    place_down = jnp.broadcast_to(place, (maxt, maxt)).T[:, :128]
    col_down = jnp.broadcast_to(coords_ref[1:2, :], (maxt, maxt)).T[:, :128]
    for low in range(0, spots, 128):
        hit = place_down == spot + low
        lists_ref[0:1, low:low + 128] = total(hit, iota((maxt, 128), 0) - maxt, 0) + maxt
        lists_ref[1:2, low:low + 128] = total(hit, col_down, 0)
        begins = total((base_down == along + low) & (need_down > 0), 1, 0)
        keep_ref[0:1, low:low + 128] = 1.0 - begins.astype(jnp.float32)
    lists_ref[2:3, 0:128] = jnp.where(slot[:, :128] < trow, last, 0)


def layer_kernel(rows_n, parts, count_hbm, coords_hbm, f_hbm, w_hbm, tiles_hbm, out_ref,
                 count_ref, coords_ref, f_ref, w_ref, tiles_ref, ft, xs, w_mine, weights, panels, spread, runs, partial, landed,
                 lists_made, keep_made, lists_ref, keep_ref,
                 local_sem, f_send, f_recv, w_send, w_recv, h_send, h_recv, sib_send, z_send, z_recv):
    me = lax.axis_index("row")
    here = lax.axis_index("col")
    maxt, tile, _ = tiles_hbm.shape
    fw, nodes = f_ref.shape
    block = nodes // rows_n
    cuts = ft.shape[0]
    cut = block // cuts
    deep = cut // tile // 2
    whole = block // tile // 2
    group = tile // fw
    rows, width = out_ref.shape
    split = width // HALF
    chunks = parts * split
    feat = rows_n * fw
    bunches = runs.shape[0] - 1
    trow = rows // tile
    core = me % 2
    sibling = me + 1 - 2 * core
    twins = rows_n // 2

    loads = [
        pltpu.make_async_copy(source, dest, local_sem.at[at]) for at, (source, dest) in enumerate((
            (f_hbm, f_ref), (w_hbm, w_ref), (coords_hbm, coords_ref), (count_hbm, count_ref),
            (tiles_hbm, tiles_ref.at[pl.ds(0, maxt)])))
    ]
    for load in loads:
        load.start()
    fetch = loads.pop()

    barrier = pltpu.get_barrier_semaphore()
    for step in range(1, rows_n):
        pl.semaphore_signal(barrier, inc=1, device_id={"row": lax.rem(me + step, rows_n)},
                            device_id_type=pl.DeviceIdType.MESH)

    @pl.when(here > 0)
    def _():
        pl.semaphore_signal(barrier, inc=1, device_id={"col": here - 1}, device_id_type=pl.DeviceIdType.MESH)

    @pl.when(here < parts - 1)
    def _():
        pl.semaphore_signal(barrier, inc=1, device_id={"col": here + 1}, device_id_type=pl.DeviceIdType.MESH)

    beside = jnp.where(here > 0, 1, 0) + jnp.where(here < parts - 1, 1, 0)
    pl.semaphore_wait(barrier, rows_n - 1 + beside)

    low_half = here < parts - 1 - here
    few = jnp.minimum(here, parts - 1 - here)

    def target(k):
        paired = k < 2 * few
        step = jnp.where(paired, k // 2, k - few)
        first = jnp.where(paired, k % 2, 0) == 0
        return jnp.where(k == parts - 1, here, jnp.where(first == low_half, parts - 1 - step, step))

    for load in loads:
        load.wait()
    for q in range(parts):
        w_mine[q] = w_ref[:, q * width:(q + 1) * width]

    def send_weight(k):
        for step in range(1, rows_n):
            remote(w_mine.at[target(k)], weights[k].at[pl.ds(pl.multiple_of(me * fw, fw), fw)],
                   w_send.at[k], w_recv.at[k], "row", lax.rem(me + step, rows_n)).start()

    send_weight(0)
    for part in range(cuts):
        for step in range(1, rows_n):
            to = lax.rem(me + step, rows_n)
            remote(f_ref.at[:, pl.ds(pl.multiple_of(to * block + part * cut, cut), cut)],
                   ft.at[part, pl.ds(pl.multiple_of(me * fw, fw), fw)],
                   f_send.at[0], f_recv.at[part, me // group], "row", to).start()

    mine = pl.ds(pl.multiple_of(me * fw, fw), fw)
    for part in range(cuts):
        ft[part, mine, :] = f_ref[:, pl.ds(pl.multiple_of(me * block + part * cut, cut), cut)]
    for k in range(parts):
        weights[k][mine, :] = w_mine[target(k)]

    tiles_ref[maxt] = jnp.zeros((tile, tile), tiles_ref.dtype)
    runs[bunches] = jnp.zeros((tile, tile), runs.dtype)
    plan(coords_ref, count_ref[0], trow, lists_made, keep_made)
    moves = [
        pltpu.make_async_copy(lists_made, lists_ref, local_sem.at[5]),
        pltpu.make_async_copy(keep_made, keep_ref, local_sem.at[6]),
    ]
    for move in moves:
        move.start()

    def others(ref, number):
        return ref.at[pl.ds(0, number)]

    def weight_of(k):
        place = others(weights[k], (rows_n - 1) * fw)
        return remote(place, place, w_send.at[k], w_recv.at[k], "row", sibling)

    groups = rows_n // group
    strip = min(cut, 512)

    def turn_in(part):
        for turn in range(groups):
            at = lax.rem(me // group + turn, groups)
            due = (group if turn else group - 1) * fw
            if due:
                place = others(ft.at[part], due)
                remote(place, place, f_send.at[0], f_recv.at[part, at], "row", sibling).wait_recv()
            lane = pl.ds(pl.multiple_of(at * tile, tile), tile)
            for low in range(0, cut, strip):
                xs[part * cut + low:part * cut + low + strip, lane] = ft[part, lane, low:low + strip].T

    def spot(c, at, part):
        if part is None:
            return panels.at[c, pl.ds(at * whole, whole)]
        return panels.at[c, pl.ds(at * whole + part * deep, deep)]

    def line_of(c, part):
        return chunks + part - 1 if part else c

    def send_chunk(c, part):
        place, line = spot(c, me, part), line_of(c, part)
        for step in range(1, twins):
            remote(place, place, h_send.at[0], h_recv.at[line, 0], "row", lax.rem(me + 2 * step, rows_n)).start()
        remote(place, place, h_send.at[0], h_recv.at[line, 1], "row", sibling).start()

    def awaited(c, part, number, way):
        place = others(panels.at[c], number * (whole if part is None else deep))
        remote(place, place, h_send.at[0], h_recv.at[line_of(c, part), way], "row", sibling).wait_recv()

    def make(k, part):
        product = jnp.dot(xs[part * cut:(part + 1) * cut, :], weights[k][...],
                          preferred_element_type=jnp.float32).astype(xs.dtype)
        for h in range(split):
            band = product[:, h * HALF:(h + 1) * HALF]
            packed = jnp.concatenate([band[:cut // 2], band[cut // 2:]], axis=1)
            panels[k * split + h, pl.ds(me * whole + part * deep, deep)] = packed.reshape(deep, tile, tile)

    def collect(c, sections):
        for part in sections:
            awaited(c, part, twins - 1, 0)
            for step in range(1, twins):
                place = spot(c, lax.rem(me + 2 * step, rows_n), part)
                remote(place, place, sib_send.at[0], h_recv.at[line_of(c, part), 1], "row", sibling).start()
        for part in sections:
            awaited(c, part, twins, 1)

    def multiply(c):
        for at in range(rows_n * whole):
            both = panels[c, at]
            low = at // deep * 2 * deep + at % deep
            spread[low] = both
            spread[low + deep] = jnp.concatenate([both[:, HALF:], both[:, :HALF]], axis=1)

        def bunch(i, total):
            left, right = [], []
            for j in range(BUNCH):
                at = i * BUNCH + j
                left.append(tiles_ref[lists_ref[0, at]])
                right.append(spread[lists_ref[1, at]])
            part = jnp.dot(jnp.concatenate(left, axis=1), jnp.concatenate(right, axis=0),
                           preferred_element_type=jnp.float32)
            total = total * keep_ref[0, i] + part
            runs[i] = total.astype(runs.dtype)
            return total

        lax.fori_loop(0, bunches, bunch, jnp.zeros((tile, tile), jnp.float32), unroll=UNROLL)
        for row in range(trow // 2):
            low = runs[lists_ref[2, row]]
            high = runs[lists_ref[2, row + trow // 2]]
            partial[c, row * tile:(row + 1) * tile, :] = jnp.concatenate([low[:, :HALF], high[:, :HALF]], axis=1)

    thick = rows // 2 // PIECES

    def piece(ref, which, p):
        return ref.at[which, pl.ds(p * thick, thick)]

    def outgoing(c, p):
        q = target(c // split)
        to = jnp.where(q > here, here + 1, here - 1)
        goes = jnp.where(q == here - 1, parts, q) * split + c % split
        return remote(piece(partial, c, p), piece(landed, goes, p), z_send.at[0], z_recv.at[goes, p],
                      "col", to)

    def stream(c):
        came = target(c // split) * split + c % split
        for p in range(PIECES):
            @pl.when((here > 0) & (here < parts - 1))
            def _():
                span = slice(p * thick, (p + 1) * thick)
                place = piece(landed, came, p)
                remote(place, place, z_send.at[0], z_recv.at[came, p], "col", here).wait_recv()
                partial[c, span, :] = (partial[c, span, :].astype(jnp.float32)
                                       + landed[came, span, :].astype(jnp.float32)).astype(partial.dtype)

            outgoing(c, p).start()

    for part in range(cuts):
        turn_in(part)
        if part == 0:
            weight_of(0).wait_recv()
        make(0, part)
        send_chunk(0, part)
    for h in range(1, split):
        send_chunk(h, None)
    for k in range(1, parts):
        send_weight(k)
    fetch.wait()
    for move in moves:
        move.wait()
    collect(0, tuple(range(cuts)))
    multiply(0)
    stream(0)
    for k in range(1, parts):
        weight_of(k).wait_recv()
        for part in range(cuts):
            make(k, part)
        for h in range(split):
            send_chunk(k * split + h, None)

    def phase(c, carry):
        collect(c, (None,))
        multiply(c)

        @pl.when(c < chunks - split)
        def _():
            stream(c)

        return carry

    lax.fori_loop(1, chunks, phase, 0)
    for p in range(PIECES):
        for h in range(split):
            span = slice(p * thick, (p + 1) * thick)
            c = chunks - split + h
            below = here * split + h
            above = parts * split + h
            for slot, there in ((below, here > 0), (above, here < parts - 1)):
                @pl.when(there)
                def _():
                    remote(piece(landed, slot, p), piece(landed, slot, p), z_send.at[0], z_recv.at[slot, p],
                           "col", here).wait_recv()

            total = partial[c, span, :].astype(jnp.float32)
            total = total + jnp.where(here > 0, landed[below, span, :].astype(jnp.float32), 0.0)
            total = total + jnp.where(here < parts - 1, landed[above, span, :].astype(jnp.float32), 0.0)
            total = total.astype(out_ref.dtype)
            high = slice(rows // 2 + p * thick, rows // 2 + (p + 1) * thick)
            out_ref[span, h * HALF:(h + 1) * HALF] = total[:, :HALF]
            out_ref[high, h * HALF:(h + 1) * HALF] = total[:, HALF:]
    for k in range(parts):
        weight_of(k).wait_send()
    place = ft.at[:, pl.ds(0, (rows_n - 1) * fw)]
    remote(place, place, f_send.at[0], f_recv.at[0, 0], "row", sibling).wait_send()
    place = panels.at[:, pl.ds(0, twins * whole)]
    remote(place, place, h_send.at[0], h_recv.at[0, 0], "row", sibling).wait_send()
    place = panels.at[:, pl.ds(0, (twins - 1) * whole)]
    remote(place, place, sib_send.at[0], h_recv.at[0, 0], "row", sibling).wait_send()
    place = partial.at[pl.ds(0, chunks - split)]
    remote(place, place, z_send.at[0], z_recv.at[0, 0], "col", here).wait_send()


def layer(features, weight_t, tiles, coords, counts, rows_n, parts):
    maxt, tile, _ = tiles.shape
    fw, nodes = features.shape
    outs = weight_t.shape[1]
    width = outs // parts
    feat = fw * rows_n
    block = nodes // rows_n
    rows = nodes * parts // rows_n
    trow = rows // tile
    bunches = maxt // BUNCH + trow * (BUNCH - 1) // BUNCH
    spots = -(-bunches * BUNCH // 128) * 128
    chunks = outs // HALF
    split = width // HALF
    cuts = min(CUTS, block // (2 * tile))
    kind = features.dtype
    vmem = pl.BlockSpec(memory_space=pltpu.VMEM)
    dma = pltpu.SemaphoreType.DMA
    return pl.pallas_call(
        functools.partial(layer_kernel, rows_n, parts),
        out_shape=jax.ShapeDtypeStruct((rows, width), kind),
        in_specs=[pl.BlockSpec(memory_space=pltpu.HBM)] * 5,
        out_specs=vmem,
        scratch_shapes=[
            pltpu.SMEM(counts.shape, jnp.int32),
            pltpu.VMEM(coords.shape, jnp.int32),
            pltpu.VMEM(features.shape, kind),
            pltpu.VMEM(weight_t.shape, kind),
            pltpu.VMEM((maxt + 1, tile, tile), kind),
            pltpu.VMEM((cuts, feat, block // cuts), kind),
            pltpu.VMEM((block, feat), kind),
            pltpu.VMEM((parts, fw, width), kind),
            [pltpu.VMEM((feat, width), kind) for _ in range(parts)],
            pltpu.VMEM((chunks, nodes // tile // 2, tile, tile), kind),
            pltpu.VMEM((nodes // tile, tile, tile), kind),
            pltpu.VMEM((bunches + 1, tile, tile), kind),
            pltpu.VMEM((chunks, rows // 2, tile), kind),
            pltpu.VMEM((chunks + split, rows // 2, tile), kind),
            pltpu.VMEM((8, spots), jnp.int32),
            pltpu.VMEM((8, spots), jnp.float32),
            pltpu.SMEM((8, spots), jnp.int32),
            pltpu.SMEM((8, spots), jnp.float32),
            dma((7,)),
            dma((1,)),
            dma((cuts, feat // tile)),
            dma((parts,)),
            dma((parts,)),
            dma((1,)),
            dma((chunks + cuts - 1, 2)),
            dma((1,)),
            dma((1,)),
            dma((chunks + split, PIECES)),
        ],
        compiler_params=pltpu.CompilerParams(
            collective_id=0, has_side_effects=True, vmem_limit_bytes=VMEM_LIMIT
        ),
        name="layer",
    )(counts, coords, features, weight_t, tiles)


def solution(mesh):
    placed = (
        P("col", "row"),
        P(None, "row"),
        P(("row", "col"), None, None),
        P(None, ("row", "col")),
        P(("row", "col")),
    )
    rows_n = mesh.shape["row"]
    parts = mesh.shape["col"]

    def body(features, weight_t, tiles, coords, counts):
        return layer(features.T, weight_t.T, tiles, coords, counts, rows_n, parts)

    return jax.shard_map(
        body, mesh=mesh, in_specs=placed, out_specs=P("row", "col"), check_vma=False
    )
```

```python
import functools

import jax
import jax.numpy as jnp
from jax import lax
from jax.experimental import pallas as pl
from jax.experimental.pallas import tpu as pltpu
from jax.sharding import PartitionSpec as P

BUNCH = 2
UNROLL = 36
CUTS = 2
PIECES = 4
HALF = 64
VMEM_LIMIT = 62 * 1024 * 1024


def remote(src, dst, send, recv, axis, to):
    return pltpu.make_async_remote_copy(
        src_ref=src,
        dst_ref=dst,
        send_sem=send,
        recv_sem=recv,
        device_id={axis: to},
        device_id_type=pl.DeviceIdType.MESH,
    )


def plan(coords_ref, count, trow, lists_ref, keep_ref):
    maxt = coords_ref.shape[1]
    spots = lists_ref.shape[1]
    bunches = maxt // BUNCH + trow * (BUNCH - 1) // BUNCH
    lists_ref[...] = jnp.zeros(lists_ref.shape, jnp.int32)
    keep_ref[...] = jnp.zeros(keep_ref.shape, jnp.float32)

    def iota(shape, axis):
        return lax.broadcasted_iota(jnp.int32, shape, axis)

    def total(mask, value, axis):
        return jnp.sum(jnp.where(mask, value, 0), axis=axis, keepdims=True, dtype=jnp.int32)

    slot = iota((1, maxt), 1)
    row = jnp.where(slot < count, coords_ref[0:1, :], 2 * trow)
    square = jnp.broadcast_to(row, (maxt, maxt))
    turned = square.T
    rank = total((square == turned) & (iota((maxt, maxt), 0) < iota((maxt, maxt), 1)), 1, 0)

    def rounds(number):
        return (number + (BUNCH - 1)) // BUNCH

    match = iota((trow, maxt), 0) == row
    need_down = rounds(total(match, 1, 1))
    spot = iota((maxt, 128), 1)
    need_along = rounds(total(turned[:, :128] == spot, 1, 0))
    down = iota((trow, 128), 0)
    along = iota((trow, 128), 1)
    base_down = total(along < down, need_along, 1)
    base_along = total(down < along, need_down, 0)
    last = jnp.where(need_along > 0, base_along + need_along - 1, bunches)
    place = jnp.where(slot < count, rank + total(match, base_down * BUNCH, 0), -1)
    place_down = jnp.broadcast_to(place, (maxt, maxt)).T[:, :128]
    col_down = jnp.broadcast_to(coords_ref[1:2, :], (maxt, maxt)).T[:, :128]
    for low in range(0, spots, 128):
        hit = place_down == spot + low
        lists_ref[0:1, low:low + 128] = total(hit, iota((maxt, 128), 0) - maxt, 0) + maxt
        lists_ref[1:2, low:low + 128] = total(hit, col_down, 0)
        begins = total((base_down == along + low) & (need_down > 0), 1, 0)
        keep_ref[0:1, low:low + 128] = 1.0 - begins.astype(jnp.float32)
    lists_ref[2:3, 0:128] = jnp.where(slot[:, :128] < trow, last, 0)


def layer_kernel(rows_n, parts, count_hbm, coords_hbm, f_hbm, w_hbm, tiles_hbm, out_ref,
                 count_ref, coords_ref, f_ref, w_ref, tiles_ref, ft, xs, w_mine, weights, panels, spread, runs, partial, landed,
                 lists_made, keep_made, lists_ref, keep_ref,
                 local_sem, f_send, f_recv, w_send, w_recv, h_send, h_recv, sib_send, z_send, z_recv):
    me = lax.axis_index("row")
    here = lax.axis_index("col")
    maxt, tile, _ = tiles_hbm.shape
    fw, nodes = f_ref.shape
    block = nodes // rows_n
    cuts = ft.shape[0]
    cut = block // cuts
    deep = cut // tile // 2
    whole = block // tile // 2
    group = tile // fw
    rows, width = out_ref.shape
    split = width // HALF
    chunks = parts * split
    feat = rows_n * fw
    bunches = runs.shape[0] - 1
    trow = rows // tile
    core = me % 2
    sibling = me + 1 - 2 * core
    twins = rows_n // 2

    loads = [
        pltpu.make_async_copy(source, dest, local_sem.at[at]) for at, (source, dest) in enumerate((
            (f_hbm, f_ref), (w_hbm, w_ref), (coords_hbm, coords_ref), (count_hbm, count_ref),
            (tiles_hbm, tiles_ref.at[pl.ds(0, maxt)])))
    ]
    for load in loads:
        load.start()
    fetch = loads.pop()

    barrier = pltpu.get_barrier_semaphore()
    for step in range(1, rows_n):
        pl.semaphore_signal(barrier, inc=1, device_id={"row": lax.rem(me + step, rows_n)},
                            device_id_type=pl.DeviceIdType.MESH)

    @pl.when(here > 0)
    def _():
        pl.semaphore_signal(barrier, inc=1, device_id={"col": here - 1}, device_id_type=pl.DeviceIdType.MESH)

    @pl.when(here < parts - 1)
    def _():
        pl.semaphore_signal(barrier, inc=1, device_id={"col": here + 1}, device_id_type=pl.DeviceIdType.MESH)

    beside = jnp.where(here > 0, 1, 0) + jnp.where(here < parts - 1, 1, 0)
    pl.semaphore_wait(barrier, rows_n - 1 + beside)

    low_half = here < parts - 1 - here
    few = jnp.minimum(here, parts - 1 - here)

    def target(k):
        paired = k < 2 * few
        step = jnp.where(paired, k // 2, k - few)
        first = jnp.where(paired, k % 2, 0) == 0
        return jnp.where(k == parts - 1, here, jnp.where(first == low_half, parts - 1 - step, step))

    for load in loads:
        load.wait()
    for q in range(parts):
        w_mine[q] = w_ref[:, q * width:(q + 1) * width]

    alike = [lax.rem(me + 2 * step, rows_n) for step in range(1, twins)]

    def send_weight(k):
        for step in range(1, rows_n):
            remote(w_mine.at[target(k)], weights[k].at[pl.ds(pl.multiple_of(me * fw, fw), fw)],
                   w_send.at[k], w_recv.at[k], "row", lax.rem(me + step, rows_n)).start()

    for to, way in [(twin, 0) for twin in alike] + [(sibling, parts)]:
        remote(w_mine.at[target(0)], weights[0].at[pl.ds(pl.multiple_of(me * fw, fw), fw)],
               w_send.at[0], w_recv.at[way], "row", to).start()
    for part in range(cuts):
        for step in range(1, rows_n):
            to = lax.rem(me + step, rows_n)
            remote(f_ref.at[:, pl.ds(pl.multiple_of(to * block + part * cut, cut), cut)],
                   ft.at[part, pl.ds(pl.multiple_of(me * fw, fw), fw)],
                   f_send.at[0], f_recv.at[part, me // group], "row", to).start()

    mine = pl.ds(pl.multiple_of(me * fw, fw), fw)
    for part in range(cuts):
        ft[part, mine, :] = f_ref[:, pl.ds(pl.multiple_of(me * block + part * cut, cut), cut)]
    for k in range(parts):
        weights[k][mine, :] = w_mine[target(k)]

    tiles_ref[maxt] = jnp.zeros((tile, tile), tiles_ref.dtype)
    runs[bunches] = jnp.zeros((tile, tile), runs.dtype)
    plan(coords_ref, count_ref[0], trow, lists_made, keep_made)
    moves = [
        pltpu.make_async_copy(lists_made, lists_ref, local_sem.at[5]),
        pltpu.make_async_copy(keep_made, keep_ref, local_sem.at[6]),
    ]
    for move in moves:
        move.start()

    def others(ref, number):
        return ref.at[pl.ds(0, number)]

    def weight_of(k, number=rows_n - 1, way=None):
        place = others(weights[k], number * fw)
        return remote(place, place, w_send.at[k], w_recv.at[k if way is None else way], "row", sibling)

    if alike:
        weight_of(0, twins - 1).wait_recv()
    for twin in alike:
        place = weights[0].at[pl.ds(pl.multiple_of(twin * fw, fw), fw)]
        remote(place, place, w_send.at[0], w_recv.at[parts], "row", sibling).start()

    groups = rows_n // group
    strip = min(cut, 512)

    def turn_in(part):
        for turn in range(groups):
            at = lax.rem(me // group + turn, groups)
            due = (group if turn else group - 1) * fw
            if due:
                place = others(ft.at[part], due)
                remote(place, place, f_send.at[0], f_recv.at[part, at], "row", sibling).wait_recv()
            lane = pl.ds(pl.multiple_of(at * tile, tile), tile)
            for low in range(0, cut, strip):
                xs[part * cut + low:part * cut + low + strip, lane] = ft[part, lane, low:low + strip].T

    def spot(c, at, part):
        if part is None:
            return panels.at[c, pl.ds(at * whole, whole)]
        return panels.at[c, pl.ds(at * whole + part * deep, deep)]

    def line_of(c, part):
        return chunks + part - 1 if part else c

    def send_chunk(c, part):
        place, line = spot(c, me, part), line_of(c, part)
        for step in range(1, twins):
            remote(place, place, h_send.at[0], h_recv.at[line, 0], "row", lax.rem(me + 2 * step, rows_n)).start()
        remote(place, place, h_send.at[0], h_recv.at[line, 1], "row", sibling).start()

    def awaited(c, part, number, way):
        place = others(panels.at[c], number * (whole if part is None else deep))
        remote(place, place, h_send.at[0], h_recv.at[line_of(c, part), way], "row", sibling).wait_recv()

    def make(k, part):
        product = jnp.dot(xs[part * cut:(part + 1) * cut, :], weights[k][...],
                          preferred_element_type=jnp.float32).astype(xs.dtype)
        for h in range(split):
            band = product[:, h * HALF:(h + 1) * HALF]
            packed = jnp.concatenate([band[:cut // 2], band[cut // 2:]], axis=1)
            panels[k * split + h, pl.ds(me * whole + part * deep, deep)] = packed.reshape(deep, tile, tile)

    def collect(c, sections):
        for part in sections:
            awaited(c, part, twins - 1, 0)
            for step in range(1, twins):
                place = spot(c, lax.rem(me + 2 * step, rows_n), part)
                remote(place, place, sib_send.at[0], h_recv.at[line_of(c, part), 1], "row", sibling).start()
        for part in sections:
            awaited(c, part, twins, 1)

    def multiply(c):
        for at in range(rows_n * whole):
            both = panels[c, at]
            low = at // deep * 2 * deep + at % deep
            spread[low] = both
            spread[low + deep] = jnp.concatenate([both[:, HALF:], both[:, :HALF]], axis=1)

        def bunch(i, total):
            left, right = [], []
            for j in range(BUNCH):
                at = i * BUNCH + j
                left.append(tiles_ref[lists_ref[0, at]])
                right.append(spread[lists_ref[1, at]])
            part = jnp.dot(jnp.concatenate(left, axis=1), jnp.concatenate(right, axis=0),
                           preferred_element_type=jnp.float32)
            total = total * keep_ref[0, i] + part
            runs[i] = total.astype(runs.dtype)
            return total

        lax.fori_loop(0, bunches, bunch, jnp.zeros((tile, tile), jnp.float32), unroll=UNROLL)
        for row in range(trow // 2):
            low = runs[lists_ref[2, row]]
            high = runs[lists_ref[2, row + trow // 2]]
            partial[c, row * tile:(row + 1) * tile, :] = jnp.concatenate([low[:, :HALF], high[:, :HALF]], axis=1)

    thick = rows // 2 // PIECES

    def piece(ref, which, p):
        return ref.at[which, pl.ds(p * thick, thick)]

    def outgoing(c, p):
        q = target(c // split)
        to = jnp.where(q > here, here + 1, here - 1)
        goes = jnp.where(q == here - 1, parts, q) * split + c % split
        return remote(piece(partial, c, p), piece(landed, goes, p), z_send.at[0], z_recv.at[goes, p],
                      "col", to)

    def stream(c):
        came = target(c // split) * split + c % split
        for p in range(PIECES):
            @pl.when((here > 0) & (here < parts - 1))
            def _():
                span = slice(p * thick, (p + 1) * thick)
                place = piece(landed, came, p)
                remote(place, place, z_send.at[0], z_recv.at[came, p], "col", here).wait_recv()
                partial[c, span, :] = (partial[c, span, :].astype(jnp.float32)
                                       + landed[came, span, :].astype(jnp.float32)).astype(partial.dtype)

            outgoing(c, p).start()

    for part in range(cuts):
        turn_in(part)
        if part == 0:
            weight_of(0, twins, parts).wait_recv()
        make(0, part)
        send_chunk(0, part)
    for h in range(1, split):
        send_chunk(h, None)
    for k in range(1, parts):
        send_weight(k)
    fetch.wait()
    for move in moves:
        move.wait()
    collect(0, tuple(range(cuts)))
    multiply(0)
    stream(0)
    for k in range(1, parts):
        weight_of(k).wait_recv()
        for part in range(cuts):
            make(k, part)
        for h in range(split):
            send_chunk(k * split + h, None)

    def phase(c, carry):
        collect(c, (None,))
        multiply(c)

        @pl.when(c < chunks - split)
        def _():
            stream(c)

        return carry

    lax.fori_loop(1, chunks, phase, 0)
    for p in range(PIECES):
        for h in range(split):
            span = slice(p * thick, (p + 1) * thick)
            c = chunks - split + h
            below = here * split + h
            above = parts * split + h
            for slot, there in ((below, here > 0), (above, here < parts - 1)):
                @pl.when(there)
                def _():
                    remote(piece(landed, slot, p), piece(landed, slot, p), z_send.at[0], z_recv.at[slot, p],
                           "col", here).wait_recv()

            total = partial[c, span, :].astype(jnp.float32)
            total = total + jnp.where(here > 0, landed[below, span, :].astype(jnp.float32), 0.0)
            total = total + jnp.where(here < parts - 1, landed[above, span, :].astype(jnp.float32), 0.0)
            total = total.astype(out_ref.dtype)
            high = slice(rows // 2 + p * thick, rows // 2 + (p + 1) * thick)
            out_ref[span, h * HALF:(h + 1) * HALF] = total[:, :HALF]
            out_ref[high, h * HALF:(h + 1) * HALF] = total[:, HALF:]
    for k in range(parts):
        weight_of(k).wait_send()
    place = ft.at[:, pl.ds(0, (rows_n - 1) * fw)]
    remote(place, place, f_send.at[0], f_recv.at[0, 0], "row", sibling).wait_send()
    place = panels.at[:, pl.ds(0, twins * whole)]
    remote(place, place, h_send.at[0], h_recv.at[0, 0], "row", sibling).wait_send()
    place = panels.at[:, pl.ds(0, (twins - 1) * whole)]
    remote(place, place, sib_send.at[0], h_recv.at[0, 0], "row", sibling).wait_send()
    place = partial.at[pl.ds(0, chunks - split)]
    remote(place, place, z_send.at[0], z_recv.at[0, 0], "col", here).wait_send()


def layer(features, weight_t, tiles, coords, counts, rows_n, parts):
    maxt, tile, _ = tiles.shape
    fw, nodes = features.shape
    outs = weight_t.shape[1]
    width = outs // parts
    feat = fw * rows_n
    block = nodes // rows_n
    rows = nodes * parts // rows_n
    trow = rows // tile
    bunches = maxt // BUNCH + trow * (BUNCH - 1) // BUNCH
    spots = -(-bunches * BUNCH // 128) * 128
    chunks = outs // HALF
    split = width // HALF
    cuts = min(CUTS, block // (2 * tile))
    kind = features.dtype
    vmem = pl.BlockSpec(memory_space=pltpu.VMEM)
    dma = pltpu.SemaphoreType.DMA
    return pl.pallas_call(
        functools.partial(layer_kernel, rows_n, parts),
        out_shape=jax.ShapeDtypeStruct((rows, width), kind),
        in_specs=[pl.BlockSpec(memory_space=pltpu.HBM)] * 5,
        out_specs=vmem,
        scratch_shapes=[
            pltpu.SMEM(counts.shape, jnp.int32),
            pltpu.VMEM(coords.shape, jnp.int32),
            pltpu.VMEM(features.shape, kind),
            pltpu.VMEM(weight_t.shape, kind),
            pltpu.VMEM((maxt + 1, tile, tile), kind),
            pltpu.VMEM((cuts, feat, block // cuts), kind),
            pltpu.VMEM((block, feat), kind),
            pltpu.VMEM((parts, fw, width), kind),
            [pltpu.VMEM((feat, width), kind) for _ in range(parts)],
            pltpu.VMEM((chunks, nodes // tile // 2, tile, tile), kind),
            pltpu.VMEM((nodes // tile, tile, tile), kind),
            pltpu.VMEM((bunches + 1, tile, tile), kind),
            pltpu.VMEM((chunks, rows // 2, tile), kind),
            pltpu.VMEM((chunks + split, rows // 2, tile), kind),
            pltpu.VMEM((8, spots), jnp.int32),
            pltpu.VMEM((8, spots), jnp.float32),
            pltpu.SMEM((8, spots), jnp.int32),
            pltpu.SMEM((8, spots), jnp.float32),
            dma((7,)),
            dma((1,)),
            dma((cuts, feat // tile)),
            dma((parts,)),
            dma((parts + 1,)),
            dma((1,)),
            dma((chunks + cuts - 1, 2)),
            dma((1,)),
            dma((1,)),
            dma((chunks + split, PIECES)),
        ],
        compiler_params=pltpu.CompilerParams(
            collective_id=0, has_side_effects=True, vmem_limit_bytes=VMEM_LIMIT
        ),
        name="layer",
    )(counts, coords, features, weight_t, tiles)


def solution(mesh):
    placed = (
        P("col", "row"),
        P(None, "row"),
        P(("row", "col"), None, None),
        P(None, ("row", "col")),
        P(("row", "col")),
    )
    rows_n = mesh.shape["row"]
    parts = mesh.shape["col"]

    def body(features, weight_t, tiles, coords, counts):
        return layer(features.T, weight_t.T, tiles, coords, counts, rows_n, parts)

    return jax.shard_map(
        body, mesh=mesh, in_specs=placed, out_specs=P("row", "col"), check_vma=False
    )
```

```python
import functools

import jax
import jax.numpy as jnp
from jax import lax
from jax.experimental import pallas as pl
from jax.experimental.pallas import tpu as pltpu
from jax.sharding import PartitionSpec as P

BUNCH = 2
UNROLL = 36
CUTS = 2
PIECES = 4
HALF = 64
VMEM_LIMIT = 62 * 1024 * 1024


def remote(src, dst, send, recv, axis, to):
    return pltpu.make_async_remote_copy(
        src_ref=src,
        dst_ref=dst,
        send_sem=send,
        recv_sem=recv,
        device_id={axis: to},
        device_id_type=pl.DeviceIdType.MESH,
    )


def plan(coords_ref, count, trow, lists_ref, keep_ref):
    maxt = coords_ref.shape[1]
    spots = lists_ref.shape[1]
    bunches = maxt // BUNCH + trow * (BUNCH - 1) // BUNCH
    lists_ref[...] = jnp.zeros(lists_ref.shape, jnp.int32)
    keep_ref[...] = jnp.zeros(keep_ref.shape, jnp.float32)

    def iota(shape, axis):
        return lax.broadcasted_iota(jnp.int32, shape, axis)

    def total(mask, value, axis):
        return jnp.sum(jnp.where(mask, value, 0), axis=axis, keepdims=True, dtype=jnp.int32)

    slot = iota((1, maxt), 1)
    row = jnp.where(slot < count, coords_ref[0:1, :], 2 * trow)
    square = jnp.broadcast_to(row, (maxt, maxt))
    turned = square.T
    rank = total((square == turned) & (iota((maxt, maxt), 0) < iota((maxt, maxt), 1)), 1, 0)

    def rounds(number):
        return (number + (BUNCH - 1)) // BUNCH

    match = iota((trow, maxt), 0) == row
    need_down = rounds(total(match, 1, 1))
    spot = iota((maxt, 128), 1)
    need_along = rounds(total(turned[:, :128] == spot, 1, 0))
    down = iota((trow, 128), 0)
    along = iota((trow, 128), 1)
    base_down = total(along < down, need_along, 1)
    base_along = total(down < along, need_down, 0)
    last = jnp.where(need_along > 0, base_along + need_along - 1, bunches)
    place = jnp.where(slot < count, rank + total(match, base_down * BUNCH, 0), -1)
    place_down = jnp.broadcast_to(place, (maxt, maxt)).T[:, :128]
    col_down = jnp.broadcast_to(coords_ref[1:2, :], (maxt, maxt)).T[:, :128]
    for low in range(0, spots, 128):
        hit = place_down == spot + low
        lists_ref[0:1, low:low + 128] = total(hit, iota((maxt, 128), 0) - maxt, 0) + maxt
        lists_ref[1:2, low:low + 128] = total(hit, col_down, 0)
        begins = total((base_down == along + low) & (need_down > 0), 1, 0)
        keep_ref[0:1, low:low + 128] = 1.0 - begins.astype(jnp.float32)
    lists_ref[2:3, 0:128] = jnp.where(slot[:, :128] < trow, last, 0)


def layer_kernel(rows_n, parts, count_hbm, coords_hbm, f_hbm, w_hbm, tiles_hbm, out_ref,
                 count_ref, coords_ref, f_ref, w_ref, tiles_ref, ft, xs, w_mine, weights, panels, spread, runs, partial, landed,
                 lists_made, keep_made, lists_ref, keep_ref,
                 local_sem, f_send, f_recv, w_send, w_recv, h_send, h_recv, sib_send, z_send, z_recv):
    me = lax.axis_index("row")
    here = lax.axis_index("col")
    maxt, tile, _ = tiles_hbm.shape
    fw, nodes = f_ref.shape
    block = nodes // rows_n
    cuts = ft.shape[0]
    cut = block // cuts
    deep = cut // tile // 2
    whole = block // tile // 2
    group = tile // fw
    rows, width = out_ref.shape
    split = width // HALF
    chunks = parts * split
    feat = rows_n * fw
    bunches = runs.shape[0] - 1
    trow = rows // tile
    core = me % 2
    sibling = me + 1 - 2 * core
    twins = rows_n // 2

    loads = [
        pltpu.make_async_copy(source, dest, local_sem.at[at]) for at, (source, dest) in enumerate((
            (f_hbm, f_ref), (w_hbm, w_ref), (coords_hbm, coords_ref), (count_hbm, count_ref),
            (tiles_hbm, tiles_ref.at[pl.ds(0, maxt)])))
    ]
    for load in loads:
        load.start()
    fetch = loads.pop()

    barrier = pltpu.get_barrier_semaphore()
    for step in range(1, rows_n):
        pl.semaphore_signal(barrier, inc=1, device_id={"row": lax.rem(me + step, rows_n)},
                            device_id_type=pl.DeviceIdType.MESH)

    @pl.when(here > 0)
    def _():
        pl.semaphore_signal(barrier, inc=1, device_id={"col": here - 1}, device_id_type=pl.DeviceIdType.MESH)

    @pl.when(here < parts - 1)
    def _():
        pl.semaphore_signal(barrier, inc=1, device_id={"col": here + 1}, device_id_type=pl.DeviceIdType.MESH)

    beside = jnp.where(here > 0, 1, 0) + jnp.where(here < parts - 1, 1, 0)
    pl.semaphore_wait(barrier, rows_n - 1 + beside)

    low_half = here < parts - 1 - here
    few = jnp.minimum(here, parts - 1 - here)

    def target(k):
        paired = k < 2 * few
        step = jnp.where(paired, k // 2, k - few)
        first = jnp.where(paired, k % 2, 0) == 0
        return jnp.where(k == parts - 1, here, jnp.where(first == low_half, parts - 1 - step, step))

    for load in loads:
        load.wait()
    for q in range(parts):
        w_mine[q] = w_ref[:, q * width:(q + 1) * width]

    alike = [lax.rem(me + 2 * step, rows_n) for step in range(1, twins)]

    def send_weight(k):
        for step in range(1, rows_n):
            remote(w_mine.at[target(k)], weights[k].at[pl.ds(pl.multiple_of(me * fw, fw), fw)],
                   w_send.at[k], w_recv.at[k], "row", lax.rem(me + step, rows_n)).start()

    for to, way in [(twin, 0) for twin in alike] + [(sibling, parts)]:
        remote(w_mine.at[target(0)], weights[0].at[pl.ds(pl.multiple_of(me * fw, fw), fw)],
               w_send.at[0], w_recv.at[way], "row", to).start()
    for part in range(cuts):
        for step in range(1, rows_n):
            to = lax.rem(me + step, rows_n)
            remote(f_ref.at[:, pl.ds(pl.multiple_of(to * block + part * cut, cut), cut)],
                   ft.at[part, pl.ds(pl.multiple_of(me * fw, fw), fw)],
                   f_send.at[0], f_recv.at[part, me // group], "row", to).start()

    mine = pl.ds(pl.multiple_of(me * fw, fw), fw)
    for part in range(cuts):
        ft[part, mine, :] = f_ref[:, pl.ds(pl.multiple_of(me * block + part * cut, cut), cut)]
    for k in range(parts):
        weights[k][mine, :] = w_mine[target(k)]

    tiles_ref[maxt] = jnp.zeros((tile, tile), tiles_ref.dtype)
    runs[bunches] = jnp.zeros((tile, tile), runs.dtype)
    plan(coords_ref, count_ref[0], trow, lists_made, keep_made)
    moves = [
        pltpu.make_async_copy(lists_made, lists_ref, local_sem.at[5]),
        pltpu.make_async_copy(keep_made, keep_ref, local_sem.at[6]),
    ]
    for move in moves:
        move.start()

    def others(ref, number):
        return ref.at[pl.ds(0, number)]

    def weight_of(k, number=rows_n - 1, way=None):
        place = others(weights[k], number * fw)
        return remote(place, place, w_send.at[k], w_recv.at[k if way is None else way], "row", sibling)

    if alike:
        weight_of(0, twins - 1).wait_recv()
    for twin in alike:
        place = weights[0].at[pl.ds(pl.multiple_of(twin * fw, fw), fw)]
        remote(place, place, w_send.at[0], w_recv.at[parts], "row", sibling).start()

    groups = rows_n // group
    strip = min(cut, 512)

    def turn_in(part):
        for turn in range(groups):
            at = lax.rem(me // group + turn, groups)
            due = (group if turn else group - 1) * fw
            if due:
                place = others(ft.at[part], due)
                remote(place, place, f_send.at[0], f_recv.at[part, at], "row", sibling).wait_recv()
            lane = pl.ds(pl.multiple_of(at * tile, tile), tile)
            for low in range(0, cut, strip):
                xs[part * cut + low:part * cut + low + strip, lane] = ft[part, lane, low:low + strip].T

    def spot(c, at, part):
        if part is None:
            return panels.at[c, pl.ds(at * whole, whole)]
        return panels.at[c, pl.ds(at * whole + part * deep, deep)]

    def line_of(c, part):
        return chunks + part - 1 if part else c

    def send_chunk(c, part):
        place, line = spot(c, me, part), line_of(c, part)
        for step in range(1, twins):
            remote(place, place, h_send.at[0], h_recv.at[line, 0], "row", lax.rem(me + 2 * step, rows_n)).start()
        remote(place, place, h_send.at[0], h_recv.at[line, 1], "row", sibling).start()

    def awaited(c, part, number, way):
        place = others(panels.at[c], number * (whole if part is None else deep))
        remote(place, place, h_send.at[0], h_recv.at[line_of(c, part), way], "row", sibling).wait_recv()

    def make(k, part):
        product = jnp.dot(xs[part * cut:(part + 1) * cut, :], weights[k][...],
                          preferred_element_type=jnp.float32).astype(xs.dtype)
        for h in range(split):
            band = product[:, h * HALF:(h + 1) * HALF]
            packed = jnp.concatenate([band[:cut // 2], band[cut // 2:]], axis=1)
            panels[k * split + h, pl.ds(me * whole + part * deep, deep)] = packed.reshape(deep, tile, tile)

    def widen(c, at, part):
        for cell in range(cuts) if part is None else (part,):
            for i in range(deep):
                both = panels[c, at * whole + cell * deep + i]
                low = (at * cuts + cell) * 2 * deep + i
                spread[low] = both
                spread[low + deep] = jnp.concatenate([both[:, HALF:], both[:, :HALF]], axis=1)

    def collect(c, sections):
        for part in sections:
            awaited(c, part, twins - 1, 0)
            for twin in alike:
                place = spot(c, twin, part)
                remote(place, place, sib_send.at[0], h_recv.at[line_of(c, part), 1], "row", sibling).start()
            for twin in [me] + alike:
                widen(c, twin, part)
        for part in sections:
            awaited(c, part, twins, 1)
            for step in range(twins):
                widen(c, lax.rem(sibling + 2 * step, rows_n), part)

    def multiply(c):
        def bunch(i, total):
            left, right = [], []
            for j in range(BUNCH):
                at = i * BUNCH + j
                left.append(tiles_ref[lists_ref[0, at]])
                right.append(spread[lists_ref[1, at]])
            part = jnp.dot(jnp.concatenate(left, axis=1), jnp.concatenate(right, axis=0),
                           preferred_element_type=jnp.float32)
            total = total * keep_ref[0, i] + part
            runs[i] = total.astype(runs.dtype)
            return total

        lax.fori_loop(0, bunches, bunch, jnp.zeros((tile, tile), jnp.float32), unroll=UNROLL)
        for row in range(trow // 2):
            low = runs[lists_ref[2, row]]
            high = runs[lists_ref[2, row + trow // 2]]
            partial[c, row * tile:(row + 1) * tile, :] = jnp.concatenate([low[:, :HALF], high[:, :HALF]], axis=1)

    thick = rows // 2 // PIECES

    def piece(ref, which, p):
        return ref.at[which, pl.ds(p * thick, thick)]

    def outgoing(c, p):
        q = target(c // split)
        to = jnp.where(q > here, here + 1, here - 1)
        goes = jnp.where(q == here - 1, parts, q) * split + c % split
        return remote(piece(partial, c, p), piece(landed, goes, p), z_send.at[0], z_recv.at[goes, p],
                      "col", to)

    def stream(c):
        came = target(c // split) * split + c % split
        for p in range(PIECES):
            @pl.when((here > 0) & (here < parts - 1))
            def _():
                span = slice(p * thick, (p + 1) * thick)
                place = piece(landed, came, p)
                remote(place, place, z_send.at[0], z_recv.at[came, p], "col", here).wait_recv()
                partial[c, span, :] = (partial[c, span, :].astype(jnp.float32)
                                       + landed[came, span, :].astype(jnp.float32)).astype(partial.dtype)

            outgoing(c, p).start()

    for part in range(cuts):
        turn_in(part)
        if part == 0:
            weight_of(0, twins, parts).wait_recv()
        make(0, part)
        send_chunk(0, part)
    for h in range(1, split):
        send_chunk(h, None)
    for k in range(1, parts):
        send_weight(k)
    fetch.wait()
    for move in moves:
        move.wait()
    collect(0, tuple(range(cuts)))
    multiply(0)
    stream(0)
    for k in range(1, parts):
        weight_of(k).wait_recv()
        for part in range(cuts):
            make(k, part)
        for h in range(split):
            send_chunk(k * split + h, None)

    def phase(c, carry):
        collect(c, (None,))
        multiply(c)

        @pl.when(c < chunks - split)
        def _():
            stream(c)

        return carry

    lax.fori_loop(1, chunks, phase, 0)
    for p in range(PIECES):
        for h in range(split):
            span = slice(p * thick, (p + 1) * thick)
            c = chunks - split + h
            below = here * split + h
            above = parts * split + h
            for slot, there in ((below, here > 0), (above, here < parts - 1)):
                @pl.when(there)
                def _():
                    remote(piece(landed, slot, p), piece(landed, slot, p), z_send.at[0], z_recv.at[slot, p],
                           "col", here).wait_recv()

            total = partial[c, span, :].astype(jnp.float32)
            total = total + jnp.where(here > 0, landed[below, span, :].astype(jnp.float32), 0.0)
            total = total + jnp.where(here < parts - 1, landed[above, span, :].astype(jnp.float32), 0.0)
            total = total.astype(out_ref.dtype)
            high = slice(rows // 2 + p * thick, rows // 2 + (p + 1) * thick)
            out_ref[span, h * HALF:(h + 1) * HALF] = total[:, :HALF]
            out_ref[high, h * HALF:(h + 1) * HALF] = total[:, HALF:]
    for k in range(parts):
        weight_of(k).wait_send()
    place = ft.at[:, pl.ds(0, (rows_n - 1) * fw)]
    remote(place, place, f_send.at[0], f_recv.at[0, 0], "row", sibling).wait_send()
    place = panels.at[:, pl.ds(0, twins * whole)]
    remote(place, place, h_send.at[0], h_recv.at[0, 0], "row", sibling).wait_send()
    place = panels.at[:, pl.ds(0, (twins - 1) * whole)]
    remote(place, place, sib_send.at[0], h_recv.at[0, 0], "row", sibling).wait_send()
    place = partial.at[pl.ds(0, chunks - split)]
    remote(place, place, z_send.at[0], z_recv.at[0, 0], "col", here).wait_send()


def layer(features, weight_t, tiles, coords, counts, rows_n, parts):
    maxt, tile, _ = tiles.shape
    fw, nodes = features.shape
    outs = weight_t.shape[1]
    width = outs // parts
    feat = fw * rows_n
    block = nodes // rows_n
    rows = nodes * parts // rows_n
    trow = rows // tile
    bunches = maxt // BUNCH + trow * (BUNCH - 1) // BUNCH
    spots = -(-bunches * BUNCH // 128) * 128
    chunks = outs // HALF
    split = width // HALF
    cuts = min(CUTS, block // (2 * tile))
    kind = features.dtype
    vmem = pl.BlockSpec(memory_space=pltpu.VMEM)
    dma = pltpu.SemaphoreType.DMA
    return pl.pallas_call(
        functools.partial(layer_kernel, rows_n, parts),
        out_shape=jax.ShapeDtypeStruct((rows, width), kind),
        in_specs=[pl.BlockSpec(memory_space=pltpu.HBM)] * 5,
        out_specs=vmem,
        scratch_shapes=[
            pltpu.SMEM(counts.shape, jnp.int32),
            pltpu.VMEM(coords.shape, jnp.int32),
            pltpu.VMEM(features.shape, kind),
            pltpu.VMEM(weight_t.shape, kind),
            pltpu.VMEM((maxt + 1, tile, tile), kind),
            pltpu.VMEM((cuts, feat, block // cuts), kind),
            pltpu.VMEM((block, feat), kind),
            pltpu.VMEM((parts, fw, width), kind),
            [pltpu.VMEM((feat, width), kind) for _ in range(parts)],
            pltpu.VMEM((chunks, nodes // tile // 2, tile, tile), kind),
            pltpu.VMEM((nodes // tile, tile, tile), kind),
            pltpu.VMEM((bunches + 1, tile, tile), kind),
            pltpu.VMEM((chunks, rows // 2, tile), kind),
            pltpu.VMEM((chunks + split, rows // 2, tile), kind),
            pltpu.VMEM((8, spots), jnp.int32),
            pltpu.VMEM((8, spots), jnp.float32),
            pltpu.SMEM((8, spots), jnp.int32),
            pltpu.SMEM((8, spots), jnp.float32),
            dma((7,)),
            dma((1,)),
            dma((cuts, feat // tile)),
            dma((parts,)),
            dma((parts + 1,)),
            dma((1,)),
            dma((chunks + cuts - 1, 2)),
            dma((1,)),
            dma((1,)),
            dma((chunks + split, PIECES)),
        ],
        compiler_params=pltpu.CompilerParams(
            collective_id=0, has_side_effects=True, vmem_limit_bytes=VMEM_LIMIT
        ),
        name="layer",
    )(counts, coords, features, weight_t, tiles)


def solution(mesh):
    placed = (
        P("col", "row"),
        P(None, "row"),
        P(("row", "col"), None, None),
        P(None, ("row", "col")),
        P(("row", "col")),
    )
    rows_n = mesh.shape["row"]
    parts = mesh.shape["col"]

    def body(features, weight_t, tiles, coords, counts):
        return layer(features.T, weight_t.T, tiles, coords, counts, rows_n, parts)

    return jax.shard_map(
        body, mesh=mesh, in_specs=placed, out_specs=P("row", "col"), check_vma=False
    )
```
